128 devices in a mesh: row: 8 (over z, x_hi), col: 16 (over y, x_lo, core).
Axes of the slice: x: 4 (x_hi: 2, x_lo: 2; x = x_hi * 2 + x_lo), y: 4, z: 4, core: 2. Of those that a mesh axis runs over, the one named last changes fastest.
Arguments:
- node_feats: bfloat16 [16384, 512], P(('row', 'col')), may hold values from -80 to 80
- block_mask: int32 [128, 128], replicated, may hold values from 0 to 1, as said below
- w_qkv: bfloat16 [2, 512, 1536], replicated, may hold values from -0.25 to 0.25
- w_out: bfloat16 [2, 512, 512], replicated, may hold values from -0.79296875 to 0.79296875
- w_up: bfloat16 [2, 512, 1024], replicated, may hold values from -0.25 to 0.25
- w_down: bfloat16 [2, 1024, 512], replicated, may hold values from -0.1875 to 0.1875
- ln_gain: float32 [2, 2, 512], replicated, may hold values from 0.1 to 1.9
- ln_bias: float32 [2, 2, 512], replicated, may hold values from -3 to 3
Outputs:
- nodes_out: bfloat16 [16384, 512], P(('row', 'col'))
The draws below stay inside these ranges and needn't reach their ends.
Inputs may be any that keep to these rules, and one draw needn't show every extreme that they name: `block_mask`: A symmetric 0/1 table over the 128 node blocks; every block is linked with itself.
All inputs are finite; a program needn't handle non-finite values.
Results may differ from the reference program's by a relative error of at most 0.022.
Values may be sent and summed in bfloat16 or wider, within the bound.
A program may use at most 128 MiB of HBM per device.

```python
import jax
import jax.numpy as jnp
from jax import lax

D = 512
HEADS = 8
FF = 1024
BLOCK = 128
LAYERS = 2
NB = 128
NODES = 16384
N_ROW = 8


def draw_node_feats(key, part):
    base = jnp.clip(jax.random.normal(key, (NODES, D), jnp.float32), -6.0, 6.0)
    return base.astype(jnp.bfloat16)


def draw_block_mask(key, part):
    index = jnp.arange(NB, dtype=jnp.int32)
    apart = jnp.abs(index[:, None] - index[None, :])
    apart = jnp.minimum(apart, NB - apart)
    random_bits = jax.random.randint(key, (NB, NB), 0, 16, dtype=jnp.int32)
    busy = jax.random.randint(jax.random.fold_in(key, 1), (NB,), 0, 8, dtype=jnp.int32) == 0
    far_row = NB // 2
    far_col = NB // (2 * N_ROW)
    limit = jnp.where(apart <= 1, 12, jnp.where(apart <= 3, 3, 0))
    limit = jnp.where(busy[:, None] | busy[None, :], jnp.maximum(limit, 2), limit)
    limit = jnp.where((apart == far_row) | (apart == far_col), 16, limit)
    upper = random_bits < limit
    linked = upper | upper.T | (apart == 0)
    return linked.astype(jnp.int32)


def scatter_about(rng, dims, scale, most, kind=jnp.bfloat16):
    array = scale * jax.random.normal(rng, dims, jnp.float32)
    return jnp.clip(array, min=-most, max=most).astype(kind)


def setup_inputs(seed: int = 0) -> dict:
    key_of = jax.random.split(jax.random.key(seed), 9)
    return {
        "node_feats": draw_node_feats(jax.random.fold_in(key_of[8], 71), 0),
        "block_mask": draw_block_mask(jax.random.fold_in(key_of[8], 71), 0),
        "w_qkv": scatter_about(key_of[2], (LAYERS, D, 3 * D), D ** -0.5, 0.25),
        "w_out": scatter_about(key_of[3], (LAYERS, D, D), (3.0 * D ** -0.5), 0.79296875),
        "w_up": scatter_about(key_of[4], (LAYERS, D, FF), D ** -0.5, 0.25),
        "w_down": scatter_about(key_of[5], (LAYERS, FF, D), FF ** -0.5, 0.1875),
        "ln_gain": jnp.clip(1.0 + 0.18 * jax.random.normal(key_of[6], (LAYERS, 2, D), jnp.float32), 0.1, 1.9),
        "ln_bias": scatter_about(key_of[7], (LAYERS, 2, D), 0.5, 3.0, jnp.float32),
    }


def layer_norm(values, gain, bias):
    center = values - lax.optimization_barrier(jnp.mean(values, axis=-1, keepdims=True))
    spread = lax.optimization_barrier(jnp.mean(center * center, axis=-1, keepdims=True))
    return center * lax.rsqrt(spread + 1e-05) * gain + bias

def attend(queries, keys, values, block_mask):
    head_dim = D // HEADS
    qrows = 512
    qsplit = queries.astype(jnp.float32).reshape(NODES // qrows, qrows, HEADS, head_dim)
    ksplit = keys.astype(jnp.float32).reshape(NODES, HEADS, head_dim)
    vsplit = values.astype(jnp.float32).reshape(NODES, HEADS, head_dim)
    mask_rows = block_mask.reshape(NODES // qrows, qrows // BLOCK, NB)

    def one_block(item):
        qblock, mblock = item
        scores = jnp.einsum('qhd,khd->hqk', qblock, ksplit) * (1.0 / head_dim ** 0.5)
        allowed = (jnp.repeat(jnp.repeat(mblock, BLOCK, axis=0), BLOCK, axis=1) > 0)[None]
        peak = lax.optimization_barrier(jnp.max(jnp.where(allowed, scores, -1e+30), axis=-1, keepdims=True))
        weights = jnp.where(allowed, jnp.exp(scores - peak), 0.0)
        mass = lax.optimization_barrier(jnp.sum(weights, axis=-1))
        rounded = lax.optimization_barrier(weights.astype(jnp.bfloat16)).astype(jnp.float32)
        summed = jnp.einsum('hqk,khd->qhd', rounded, vsplit)
        return (summed / mass.T[:, :, None]).reshape(qrows, D).astype(jnp.bfloat16)
    return lax.map(one_block, (qsplit, mask_rows)).reshape(NODES, D)

def reference(node_feats, block_mask, w_qkv, w_out, w_up, w_down, ln_gain, ln_bias):
    x = node_feats
    for layer in range(LAYERS):
        qkv = jnp.dot(x, w_qkv[layer], preferred_element_type=jnp.float32).astype(jnp.bfloat16)
        attn = attend(qkv[:, :D], qkv[:, D:2 * D], qkv[:, 2 * D:], block_mask)
        mixed = jnp.dot(attn, w_out[layer], preferred_element_type=jnp.float32)
        hidden = layer_norm(x.astype(jnp.float32) + mixed, ln_gain[layer, 0], ln_bias[layer, 0]).astype(jnp.bfloat16)
        up = jax.nn.gelu(jnp.dot(hidden, w_up[layer], preferred_element_type=jnp.float32)).astype(jnp.bfloat16)
        down = jnp.dot(up, w_down[layer], preferred_element_type=jnp.float32)
        x = layer_norm(hidden.astype(jnp.float32) + down, ln_gain[layer, 1], ln_bias[layer, 1]).astype(jnp.bfloat16)
    return x
```

```python
import functools

import jax
import jax.numpy as jnp
from jax import lax
from jax.experimental import pallas as pl
from jax.experimental.pallas import tpu as pltpu
from jax.sharding import PartitionSpec as P

HEADS = 8
BLOCK = 128
LAYERS = 2
NQ = 8
NK = 16
LOG2E = 1.4426950408889634
LOW = -1e30


def dot_nn(a, b):
    return lax.dot_general(a, b, (((1,), (0,)), ((), ())), preferred_element_type=jnp.float32)


def dot_nt(a, b):
    return lax.dot_general(a, b, (((1,), (1,)), ((), ())), preferred_element_type=jnp.float32)


def layer_norm(values, gain, bias):
    center = values - jnp.mean(values, axis=-1, keepdims=True)
    spread = jnp.mean(center * center, axis=-1, keepdims=True)
    return center * lax.rsqrt(spread + 1e-05) * gain + bias


def attention_kernel(sub_ref, q_ref, k_ref, vt_ref, a_ref, lse_ref, order, qd, acc):
    qd[...] = jnp.zeros_like(qd)

    def one_query_block(r, carry):
        count = jnp.int32(0)
        for k in range(NK):
            order[count] = k
            count = count + sub_ref[r, k]
        for p in range(4):
            qd[p, 0:64, 0:128] = q_ref[r, 128 * p : 128 * p + 64, :]
            qd[p, 64:128, 128:256] = q_ref[r, 128 * p + 64 : 128 * p + 128, :]
        acc[...] = jnp.zeros_like(acc)

        def step(blocks, state):
            out = []
            for p in range(4):
                peak, mass = state[p]
                lanes = slice(128 * p, 128 * p + 128)
                keys = jnp.concatenate([k_ref[b, :, lanes] for b in blocks], axis=0)
                s = dot_nn(keys, qd[p])
                top = jnp.maximum(peak, jnp.max(s, axis=0, keepdims=True))
                fade = jnp.exp2(peak - top)
                w = jnp.exp2(s - top)
                mass = mass * fade + jnp.sum(w, axis=0, keepdims=True)
                values = jnp.concatenate([vt_ref[b, lanes, :] for b in blocks], axis=1)
                o = dot_nn(values, w.astype(jnp.bfloat16))
                lo, hi = slice(128 * p, 128 * p + 64), slice(128 * p + 64, 128 * p + 128)
                acc[lo, :] = acc[lo, :] * fade[:, :128] + o[0:64, 0:128]
                acc[hi, :] = acc[hi, :] * fade[:, 128:] + o[64:128, 128:256]
                out.append((top, mass))
            return tuple(out)

        def pair(i, state):
            return step((order[2 * i], order[2 * i + 1]), state)

        start = tuple(
            (jnp.full((1, 256), LOW, jnp.float32), jnp.zeros((1, 256), jnp.float32))
            for _ in range(4)
        )
        state = lax.fori_loop(0, count // 2, pair, start)
        state = lax.cond(
            count % 2 == 1, lambda s: step((order[jnp.maximum(count - 1, 0)],), s), lambda s: s, state
        )
        for p in range(4):
            peak, mass = state[p]
            some = mass > 0.0
            inv = jnp.where(some, 1.0 / jnp.where(some, mass, 1.0), 0.0)
            lse = jnp.where(some, peak + jnp.log2(jnp.where(some, mass, 1.0)), LOW)
            for h in range(2):
                rows = slice(128 * p + 64 * h, 128 * p + 64 * h + 64)
                side = slice(128 * h, 128 * h + 128)
                a_ref[r, rows, :] = (acc[rows, :] * inv[:, side]).astype(jnp.bfloat16)
                lse_ref[r, 2 * p + h : 2 * p + h + 1, :] = lse[:, side]
        return carry

    lax.fori_loop(0, NQ, one_query_block, 0)


def attention(sub, q, k, vt):
    vmem = pl.BlockSpec(memory_space=pltpu.VMEM)
    return pl.pallas_call(
        attention_kernel,
        out_shape=(
            jax.ShapeDtypeStruct((NQ, 512, 128), jnp.bfloat16),
            jax.ShapeDtypeStruct((NQ, HEADS, 128), jnp.float32),
        ),
        in_specs=[pl.BlockSpec(memory_space=pltpu.SMEM), vmem, vmem, vmem],
        out_specs=(vmem, vmem),
        scratch_shapes=[
            pltpu.SMEM((NK + 1,), jnp.int32),
            pltpu.VMEM((4, 128, 256), jnp.bfloat16),
            pltpu.VMEM((512, 128), jnp.float32),
        ],
    )(sub, q, k, vt)


def per_device(node_feats, block_mask, w_qkv, w_out, w_up, w_down, ln_gain, ln_bias):
    rows, width = node_feats.shape
    row = lax.axis_index("row")
    col = lax.axis_index("col")
    sub = lax.dynamic_index_in_dim(block_mask.reshape(NQ, NK, NQ * NK), col, 1, keepdims=False)
    sub = lax.dynamic_slice_in_dim(sub, row * NK, NK, 1)
    x = node_feats
    for layer in range(LAYERS):
        w = w_qkv[layer]
        qt = (dot_nt(w[:, :width].T, x) * (0.125 * LOG2E)).astype(jnp.bfloat16)
        gathered = lax.all_gather(x, "col", axis=0, tiled=True)
        k = dot_nn(gathered, w[:, width : 2 * width]).astype(jnp.bfloat16).reshape(NK, 128, width)
        vt = jnp.einsum(
            "bni,io->bon", gathered.reshape(NK, 128, width), w[:, 2 * width :],
            preferred_element_type=jnp.float32,
        ).astype(jnp.bfloat16)
        q = lax.all_gather(qt, "row", axis=0, tiled=False)
        a, lse = attention(sub, q, k, vt)
        a = lax.all_to_all(a, "row", 0, 0, tiled=True)
        lse = lax.all_to_all(lse, "row", 0, 0, tiled=True)
        part = jnp.exp2(lse - jnp.max(lse, axis=0, keepdims=True))
        part = part / jnp.sum(part, axis=0, keepdims=True)
        attn = jnp.sum(
            a.reshape(NQ, HEADS, 64, 128).astype(jnp.float32) * part[:, :, None, :], axis=0
        )
        attn = attn.reshape(width, 128).astype(jnp.bfloat16).T
        mixed = jnp.dot(attn, w_out[layer], preferred_element_type=jnp.float32)
        hidden = layer_norm(
            x.astype(jnp.float32) + mixed, ln_gain[layer, 0], ln_bias[layer, 0]
        ).astype(jnp.bfloat16)
        up = jax.nn.gelu(jnp.dot(hidden, w_up[layer], preferred_element_type=jnp.float32)).astype(
            jnp.bfloat16
        )
        down = jnp.dot(up, w_down[layer], preferred_element_type=jnp.float32)
        x = layer_norm(
            hidden.astype(jnp.float32) + down, ln_gain[layer, 1], ln_bias[layer, 1]
        ).astype(jnp.bfloat16)
    return x


def solution(mesh):
    placed = (P(("row", "col"), None), P(), P(), P(), P(), P(), P(), P())
    return jax.shard_map(
        per_device, mesh=mesh, in_specs=placed, out_specs=P(("row", "col"), None), check_vma=False
    )
```

```python
import functools

import jax
import jax.numpy as jnp
from jax import lax
from jax.experimental import pallas as pl
from jax.experimental.pallas import tpu as pltpu
from jax.sharding import PartitionSpec as P

HEADS = 8
BLOCK = 128
LAYERS = 2
NQ = 8
NK = 16
LOG2E = 1.4426950408889634
LOW = -1e30
HALF = 64
PACK = 272
MESH = pl.DeviceIdType.MESH


def dot_nn(a, b):
    return lax.dot_general(a, b, (((1,), (0,)), ((), ())), preferred_element_type=jnp.float32)


def dot_nt(a, b):
    return lax.dot_general(a, b, (((1,), (1,)), ((), ())), preferred_element_type=jnp.float32)


def layer_norm(values, gain, bias):
    center = values - jnp.mean(values, axis=-1, keepdims=True)
    spread = jnp.mean(center * center, axis=-1, keepdims=True)
    return center * lax.rsqrt(spread + 1e-05) * gain + bias


def split_lse(lse):
    high = lse.astype(jnp.bfloat16).astype(jnp.float32)
    rest = lse - high
    mid = rest.astype(jnp.bfloat16).astype(jnp.float32)
    low = rest - mid
    return jnp.concatenate([high, mid, low, jnp.zeros_like(low)], axis=0).astype(jnp.bfloat16)


def joined_lse(ref):
    parts = ref[256:272, :].astype(jnp.float32)
    return parts[0:4] + parts[4:8] + parts[8:12]


def attention_kernel(sub_ref, q_ref, k_ref, vt_ref, a_ref, order, qd, acc):
    qd[...] = jnp.zeros_like(qd)

    def one_query_block(r, carry):
        count = jnp.int32(0)
        for k in range(NK):
            order[count] = k
            count = count + sub_ref[r, k]
        for p in range(4):
            qd[p, 0:64, 0:128] = q_ref[r, 128 * p : 128 * p + 64, :]
            qd[p, 64:128, 128:256] = q_ref[r, 128 * p + 64 : 128 * p + 128, :]
        acc[...] = jnp.zeros_like(acc)

        def step(blocks, state):
            out = []
            for p in range(4):
                peak, mass = state[p]
                lanes = slice(128 * p, 128 * p + 128)
                keys = jnp.concatenate([k_ref[b, :, lanes] for b in blocks], axis=0)
                s = dot_nn(keys, qd[p])
                top = jnp.maximum(peak, jnp.max(s, axis=0, keepdims=True))
                fade = jnp.exp2(peak - top)
                w = jnp.exp2(s - top)
                mass = mass * fade + jnp.sum(w, axis=0, keepdims=True)
                values = jnp.concatenate([vt_ref[b, lanes, :] for b in blocks], axis=1)
                o = dot_nn(values, w.astype(jnp.bfloat16))
                lo, hi = slice(128 * p, 128 * p + 64), slice(128 * p + 64, 128 * p + 128)
                acc[lo, :] = acc[lo, :] * fade[:, :128] + o[0:64, 0:128]
                acc[hi, :] = acc[hi, :] * fade[:, 128:] + o[64:128, 128:256]
                out.append((top, mass))
            return tuple(out)

        def pair(i, state):
            return step((order[2 * i], order[2 * i + 1]), state)

        start = tuple(
            (jnp.full((1, 256), LOW, jnp.float32), jnp.zeros((1, 256), jnp.float32))
            for _ in range(4)
        )
        state = lax.fori_loop(0, count // 2, pair, start)
        state = lax.cond(
            count % 2 == 1, lambda s: step((order[jnp.maximum(count - 1, 0)],), s), lambda s: s, state
        )
        for half in range(2):
            found = []
            for p in (2 * half, 2 * half + 1):
                peak, mass = state[p]
                some = mass > 0.0
                safe = jnp.where(some, mass, 1.0)
                inv = jnp.where(some, 1.0 / safe, 0.0)
                lse = jnp.where(some, peak + jnp.log2(safe), LOW)
                for h in range(2):
                    rows = slice(128 * p + 64 * h, 128 * p + 64 * h + 64)
                    here = slice(128 * (p % 2) + 64 * h, 128 * (p % 2) + 64 * h + 64)
                    side = slice(128 * h, 128 * h + 128)
                    a_ref[r, half, here, :] = (acc[rows, :] * inv[:, side]).astype(jnp.bfloat16)
                    found.append(lse[:, side])
            a_ref[r, half, 256:272, :] = split_lse(jnp.concatenate(found, axis=0))
        return carry

    lax.fori_loop(0, NQ, one_query_block, 0)


def attention(sub, q, k, vt):
    vmem = pl.BlockSpec(memory_space=pltpu.VMEM)
    return pl.pallas_call(
        attention_kernel,
        out_shape=jax.ShapeDtypeStruct((NQ, 2, PACK, 128), jnp.bfloat16),
        in_specs=[pl.BlockSpec(memory_space=pltpu.SMEM), vmem, vmem, vmem],
        out_specs=vmem,
        scratch_shapes=[
            pltpu.SMEM((NK + 1,), jnp.int32),
            pltpu.VMEM((4, 128, 256), jnp.bfloat16),
            pltpu.VMEM((512, 128), jnp.float32),
        ],
    )(sub, q, k, vt)


class Place:
    def __init__(self):
        row, col = lax.axis_index("row"), lax.axis_index("col")
        self.z, self.y, self.core = row // 2, col // 4, col % 2
        self.x = (row % 2) * 2 + (col // 2) % 2

    def at(self, x=None, y=None, z=None, core=None):
        x = self.x if x is None else x
        y = self.y if y is None else y % 4
        z = self.z if z is None else z % 4
        core = self.core if core is None else core
        return (z * 2 + x // 2, (y * 2 + x % 2) * 2 + core)


def key_blocks(place):
    out = []
    for c in range(2):
        for dx in range(2):
            for dy in range(4):
                x = place.x if dx == 0 else place.x + 1 - 2 * (place.x % 2)
                core = place.core if c == 0 else 1 - place.core
                row, col = place.at(x=x, y=place.y + dy, core=core)
                out.append(row * 16 + col)
    return out


def query_blocks(place):
    out = []
    for dx in range(2):
        for dz in range(4):
            x = place.x if dx == 0 else 3 - place.x
            row, col = place.at(x=x, z=place.z + dz)
            out.append(row * 16 + col)
    return out


class Wire:
    def __init__(self, send_sem, recv_sem):
        self.send_sem, self.recv_sem, self.copies = send_sem, recv_sem, {}

    def send(self, name, src, dst, to):
        m = len(self.copies)
        copy = pltpu.make_async_remote_copy(
            src_ref=src,
            dst_ref=dst,
            send_sem=self.send_sem.at[m],
            recv_sem=self.recv_sem.at[m],
            device_id=to,
            device_id_type=MESH,
        )
        copy.start()
        self.copies[name] = copy

    def arrived(self, name):
        self.copies[name].wait_recv()

    def drain(self):
        for copy in self.copies.values():
            copy.wait_send()


def merged(refs):
    lses = [joined_lse(ref) for ref in refs]
    top = functools.reduce(jnp.maximum, lses)
    parts = [jnp.exp2(lse - top) for lse in lses]
    total = functools.reduce(jnp.add, parts)
    shares = [part / total for part in parts]
    heads = []
    for h in range(4):
        rows = slice(64 * h, 64 * h + 64)
        heads.append(
            functools.reduce(
                jnp.add,
                [ref[rows, :].astype(jnp.float32) * s[h : h + 1, :] for ref, s in zip(refs, shares)],
            )
        )
    return heads, top + jnp.log2(total)


def merge_into(out, refs):
    heads, lse = merged(refs)
    for h in range(4):
        out[64 * h : 64 * h + 64, :] = heads[h].astype(jnp.bfloat16)
    out[256:272, :] = split_lse(lse)


def reduce_and_mix(wire, peers, a, got, mix, x_ref, weights, gain, bias, spare):
    zp, zm, xq = peers
    w_out, w_up, w_down, ready = weights
    slot = lambda dx, dz, h: a.at[dx * 4 + dz, h]
    for h in range(2):
        wire.send(("x2", h), slot(1, 2, h), got.at[h], xq)
    for h in range(2):
        wire.send(("pm", h), slot(1, 1, h), got.at[2 + h], zp)
        wire.send(("mm", h), slot(1, 3, h), got.at[4 + h], zm)
    wire.arrived(("x2", 0))
    merge_into(mix.at[0], [got.at[0], slot(0, 2, 0)])
    wire.send("cp", mix.at[0], got.at[6], zp)
    wire.arrived(("x2", 1))
    merge_into(mix.at[1], [got.at[1], slot(0, 2, 1)])
    wire.send("cm", mix.at[1], got.at[7], zm)
    wire.send(("zp", 1), slot(0, 1, 1), got.at[8], zp)
    wire.send(("zm", 0), slot(0, 3, 0), got.at[9], zm)
    for h in range(2):
        wire.arrived(("pm", h))
        wire.arrived(("mm", h))
        merge_into(mix.at[2 + h], [got.at[2 + h], got.at[4 + h], slot(1, 0, h)])
        wire.send(("x", h), mix.at[2 + h], got.at[10 + h], xq)
    wire.arrived("cp")
    merge_into(mix.at[4], [got.at[6], slot(0, 1, 0)])
    wire.send(("zp", 0), mix.at[4], got.at[12], zp)
    wire.arrived("cm")
    merge_into(mix.at[5], [got.at[7], slot(0, 3, 1)])
    wire.send(("zm", 1), mix.at[5], got.at[13], zm)
    ends = {0: (12, 9, 10), 1: (8, 13, 11)}
    for h in (1, 0):
        for name in (("zp", h), ("zm", h), ("x", h)):
            wire.arrived(name)
        heads, _ = merged([got.at[i] for i in ends[h]] + [slot(0, 0, h)])
        for i in range(4):
            spare[256 * h + 64 * i : 256 * h + 64 * i + 64, :] = heads[i]
    for i in ready:
        i.wait()
    attn = jnp.concatenate(
        [jnp.transpose(spare[128 * i : 128 * i + 128, :]) for i in range(4)], axis=1
    ).astype(jnp.bfloat16)
    mixed = dot_nn(attn, w_out[...])
    hidden = layer_norm(x_ref[...].astype(jnp.float32) + mixed, gain[0:1], bias[0:1]).astype(jnp.bfloat16)
    up = jax.nn.gelu(dot_nn(hidden, w_up[...])).astype(jnp.bfloat16)
    down = dot_nn(up, w_down[...])
    return layer_norm(hidden.astype(jnp.float32) + down, gain[1:2], bias[1:2]).astype(jnp.bfloat16)


def gather_and_project(wire, peers, x_ref, xg, qg, w, wvt, ready, q_ref, k_ref, vt_ref):
    zp, zm, xq, yp, ym, xk, sib = peers

    def part(ref, h):
        return ref.at[pl.ds(HALF * h, HALF)]

    def key(c, dx, dy, h):
        return xg.at[c * 8 + dx * 4 + dy, pl.ds(HALF * h, HALF)]

    def query(dx, dz, h):
        return qg.at[dx * 4 + dz, pl.ds(256 * h, 256)]

    for h in range(2):
        wire.send(("k", 0, 3, h), part(x_ref, h), key(0, 0, 3, h), yp)
        wire.send(("k", 0, 1, 1 - h), part(x_ref, 1 - h), key(0, 0, 1, 1 - h), ym)
        wire.send(("k", 1, 0, h), part(x_ref, h), key(0, 1, 0, h), xk)
    for h in range(2):
        wire.send(("s", 0, 0, h), part(x_ref, h), key(1, 0, 0, h), sib)
    for i in ready:
        i.wait()
    q = dot_nn(x_ref[...], w[:, 0:512]) * (0.125 * LOG2E)
    for i in range(4):
        qg[0, 128 * i : 128 * i + 128, :] = jnp.transpose(q[:, 128 * i : 128 * i + 128]).astype(
            jnp.bfloat16
        )
    for h in range(2):
        wire.send(("q", 0, 3, h), query(0, 0, h), query(0, 3, h), zp)
        wire.send(("q", 0, 1, 1 - h), query(0, 0, 1 - h), query(0, 1, 1 - h), zm)
        wire.send(("q", 1, 0, h), query(0, 0, h), query(1, 0, h), xq)
    wvt[...] = jnp.transpose(w[:, 1024:1536].astype(jnp.float32)).astype(jnp.bfloat16)

    def project(slots):
        rows = jnp.concatenate(
            [x_ref[...] if s == 0 else xg[s] for s in slots], axis=0
        )
        keys = dot_nn(rows, w[:, 512:1024]).astype(jnp.bfloat16)
        values = dot_nt(wvt[...], rows).astype(jnp.bfloat16)
        for i, s in enumerate(slots):
            k_ref[s] = keys[128 * i : 128 * i + 128]
            vt_ref[s] = values[:, 128 * i : 128 * i + 128]

    def across(dx, dy, h):
        wire.send(("s", dx, dy, h), key(0, dx, dy, h), key(1, dx, dy, h), sib)

    wire.arrived(("k", 0, 3, 0))
    wire.send(("k", 0, 2, 0), key(0, 0, 3, 0), key(0, 0, 2, 0), yp)
    across(0, 3, 0)
    wire.arrived(("k", 0, 1, 1))
    wire.send(("k", 0, 2, 1), key(0, 0, 1, 1), key(0, 0, 2, 1), ym)
    across(0, 1, 1)
    wire.arrived(("k", 1, 0, 0))
    wire.send(("k", 1, 3, 0), key(0, 1, 0, 0), key(0, 1, 3, 0), yp)
    wire.send(("k", 1, 1, 0), key(0, 1, 0, 0), key(0, 1, 1, 0), ym)
    across(1, 0, 0)
    wire.arrived(("q", 0, 3, 0))
    wire.send(("q", 0, 2, 0), query(0, 3, 0), query(0, 2, 0), zp)
    wire.arrived(("q", 0, 1, 1))
    wire.send(("q", 0, 2, 1), query(0, 1, 1), query(0, 2, 1), zm)
    wire.arrived(("q", 1, 0, 0))
    wire.send(("q", 1, 3, 0), query(1, 0, 0), query(1, 3, 0), zp)
    wire.send(("q", 1, 1, 0), query(1, 0, 0), query(1, 1, 0), zm)
    wire.arrived(("k", 1, 0, 1))
    wire.send(("k", 1, 3, 1), key(0, 1, 0, 1), key(0, 1, 3, 1), yp)
    wire.send(("k", 1, 1, 1), key(0, 1, 0, 1), key(0, 1, 1, 1), ym)
    across(1, 0, 1)
    wire.arrived(("k", 0, 3, 1))
    across(0, 3, 1)
    wire.arrived(("k", 0, 1, 0))
    across(0, 1, 0)
    for h in range(2):
        wire.arrived(("s", 0, 0, h))
    project((0, 8))
    wire.arrived(("q", 1, 0, 1))
    wire.send(("q", 1, 3, 1), query(1, 0, 1), query(1, 3, 1), zp)
    wire.send(("q", 1, 1, 1), query(1, 0, 1), query(1, 1, 1), zm)
    wire.arrived(("q", 0, 3, 1))
    wire.arrived(("q", 0, 1, 0))
    for h in range(2):
        wire.arrived(("k", 0, 2, h))
        wire.send(("k", 1, 2, h), key(0, 0, 2, h), key(0, 1, 2, h), xk)
        across(0, 2, h)
    project((1, 3))
    for h in range(2):
        wire.arrived(("q", 0, 2, h))
        wire.send(("q", 1, 2, h), query(0, 2, h), query(1, 2, h), xq)
    project((2, 4))
    for h in range(2):
        wire.arrived(("k", 1, 3, h))
        across(1, 3, h)
        wire.arrived(("k", 1, 1, h))
        across(1, 1, h)
    for h in range(2):
        for dy in (1, 3):
            wire.arrived(("s", 0, dy, h))
    project((9, 11))
    project((5, 7))
    for h in range(2):
        wire.arrived(("k", 1, 2, h))
        across(1, 2, h)
    for h in range(2):
        wire.arrived(("s", 0, 2, h))
        wire.arrived(("s", 1, 0, h))
    project((10, 12))
    for h in range(2):
        for dy in (1, 3):
            wire.arrived(("s", 1, dy, h))
    project((13, 15))
    for h in range(2):
        wire.arrived(("s", 1, 2, h))
    project((6, 14))
    for dz in (1, 2, 3):
        for h in range(2):
            wire.arrived(("q", 1, dz, h))
    q_ref[...] = qg[...]


def link_kernel(layer, reduces, gathers, *refs):
    refs = list(refs)
    x_ref = refs.pop(0)
    if reduces:
        a_ref, w_out_h, w_up_h, w_down_h, gain_ref, bias_ref = refs[:6]
        refs = refs[6:]
    if gathers:
        w_h = refs.pop(0)
    if reduces:
        x_out = refs.pop(0)
    if gathers:
        q_ref, k_ref, vt_ref = refs[:3]
        refs = refs[3:]
    send_sem, recv_sem, copy_sem = refs[:3]
    refs = refs[3:]
    place = Place()
    peers = [
        place.at(z=place.z + 1),
        place.at(z=place.z + 3),
        place.at(x=3 - place.x),
    ]
    if gathers:
        peers += [
            place.at(y=place.y + 1),
            place.at(y=place.y + 3),
            place.at(x=place.x + 1 - 2 * (place.x % 2)),
            place.at(core=1 - place.core),
        ]
    copies = []

    def load(src, dst):
        copy = pltpu.make_async_copy(src, dst, copy_sem.at[len(copies)])
        copy.start()
        copies.append(copy)
        return copy

    if reduces:
        got, mix, spare, w_out, w_up, w_down = refs[:6]
        refs = refs[6:]
        mix_ready = [
            load(w_out_h.at[layer], w_out),
            load(w_up_h.at[layer], w_up),
            load(w_down_h.at[layer], w_down),
        ]
    if gathers:
        xg, qg, w, wvt = refs
        w_ready = [load(w_h.at[layer + 1], w)]
    barrier = pltpu.get_barrier_semaphore()
    for peer in peers:
        pl.semaphore_signal(barrier, inc=1, device_id=peer, device_id_type=MESH)
    pl.semaphore_wait(barrier, len(peers))
    wire = Wire(send_sem, recv_sem)
    if reduces:
        x_out[...] = reduce_and_mix(
            wire, peers[:3], a_ref, got, mix, x_ref, (w_out, w_up, w_down, mix_ready),
            gain_ref[layer], bias_ref[layer], spare,
        )
        x_ref = x_out
    if gathers:
        gather_and_project(wire, peers, x_ref, xg, qg, w, wvt, w_ready, q_ref, k_ref, vt_ref)
    wire.drain()


def link(layer, x, reduce_args=None, w_qkv=None):
    reduces, gathers = reduce_args is not None, w_qkv is not None
    vmem = pl.BlockSpec(memory_space=pltpu.VMEM)
    hbm = pl.BlockSpec(memory_space=pl.ANY)
    args, specs, outs = [x], [vmem], []
    scratch = [
        pltpu.SemaphoreType.DMA((14 * reduces + 44 * gathers,)),
        pltpu.SemaphoreType.DMA((14 * reduces + 44 * gathers,)),
        pltpu.SemaphoreType.DMA((4,)),
    ]
    bf16 = jnp.bfloat16
    if reduces:
        args += list(reduce_args)
        specs += [vmem, hbm, hbm, hbm, vmem, vmem]
        outs.append(jax.ShapeDtypeStruct((128, 512), bf16))
        scratch += [
            pltpu.VMEM((14, PACK, 128), bf16),
            pltpu.VMEM((6, PACK, 128), bf16),
            pltpu.VMEM((512, 128), jnp.float32),
            pltpu.VMEM((512, 512), bf16),
            pltpu.VMEM((512, 1024), bf16),
            pltpu.VMEM((1024, 512), bf16),
        ]
    if gathers:
        args.append(w_qkv)
        specs.append(hbm)
        outs += [
            jax.ShapeDtypeStruct((NQ, 512, 128), bf16),
            jax.ShapeDtypeStruct((NK, 128, 512), bf16),
            jax.ShapeDtypeStruct((NK, 512, 128), bf16),
        ]
        scratch += [
            pltpu.VMEM((NK, 128, 512), bf16),
            pltpu.VMEM((NQ, 512, 128), bf16),
            pltpu.VMEM((512, 1536), bf16),
            pltpu.VMEM((512, 512), bf16),
        ]
    return pl.pallas_call(
        functools.partial(link_kernel, layer, reduces, gathers),
        out_shape=tuple(outs),
        in_specs=specs,
        out_specs=tuple(vmem for _ in outs),
        scratch_shapes=scratch,
        compiler_params=pltpu.CompilerParams(collective_id=layer + 1, has_side_effects=True),
    )(*args)


def per_device(node_feats, block_mask, w_qkv, w_out, w_up, w_down, ln_gain, ln_bias):
    place = Place()
    queries = jnp.stack(query_blocks(place))
    keys = jnp.stack(key_blocks(place))
    sub = block_mask[queries[:, None], keys[None, :]]
    x = node_feats
    q, k, vt = link(-1, x, w_qkv=w_qkv)
    for layer in range(LAYERS):
        parts = attention(sub, q, k, vt)
        last = layer == LAYERS - 1
        rest = (parts, w_out, w_up, w_down, ln_gain, ln_bias)
        if last:
            (x,) = link(layer, x, reduce_args=rest)
        else:
            x, q, k, vt = link(layer, x, reduce_args=rest, w_qkv=w_qkv)
    return x


def solution(mesh):
    placed = (P(("row", "col"), None), P(), P(), P(), P(), P(), P(), P())
    return jax.shard_map(
        per_device, mesh=mesh, in_specs=placed, out_specs=P(("row", "col"), None), check_vma=False
    )
```

```python
import functools

import jax
import jax.numpy as jnp
from jax import lax
from jax.experimental import pallas as pl
from jax.experimental.pallas import tpu as pltpu
from jax.sharding import PartitionSpec as P

HEADS = 8
BLOCK = 128
LAYERS = 2
NQ = 8
NK = 16
LOG2E = 1.4426950408889634
LOW = -1e30
HALF = 64
PACK = 272
MESH = pl.DeviceIdType.MESH


def dot_nn(a, b):
    return lax.dot_general(a, b, (((1,), (0,)), ((), ())), preferred_element_type=jnp.float32)


def dot_nt(a, b):
    return lax.dot_general(a, b, (((1,), (1,)), ((), ())), preferred_element_type=jnp.float32)


def layer_norm(values, gain, bias):
    center = values - jnp.mean(values, axis=-1, keepdims=True)
    spread = jnp.mean(center * center, axis=-1, keepdims=True)
    return center * lax.rsqrt(spread + 1e-05) * gain + bias


def split_lse(lse):
    high = lse.astype(jnp.bfloat16).astype(jnp.float32)
    rest = lse - high
    mid = rest.astype(jnp.bfloat16).astype(jnp.float32)
    low = rest - mid
    return jnp.concatenate([high, mid, low, jnp.zeros_like(low)], axis=0).astype(jnp.bfloat16)


def joined_lse(ref):
    parts = ref[256:272, :].astype(jnp.float32)
    return parts[0:4] + parts[4:8] + parts[8:12]


def attention_kernel(sub_ref, qd, k_ref, vt_ref, a_ref, order, scores_a, scores_b, tops_a, tops_b, peaks, masses, acc):
    bank = ((scores_a, tops_a), (scores_b, tops_b))
    count = jnp.int32(0)
    for r in range(NQ):
        for k in range(NK):
            order[count] = 32 * r + k
            count = count + sub_ref[r, k]
        order[count] = order[jnp.maximum(count - 1, 0)] + 16
        count = count + count % 2
    units = count // 2
    last = jnp.maximum(count - 1, 0)
    tail = order[last]
    order[count] = tail - tail % 32 + tail % 16 + 16
    order[count + 1] = order[count]
    peaks[...] = jnp.full_like(peaks, LOW)
    masses[...] = jnp.zeros_like(masses)
    acc[...] = jnp.zeros_like(acc)

    def decode(u):
        first, second = order[2 * u], order[2 * u + 1]
        dead = [jnp.where((code // 16) % 2 == 1, LOW, 0.0) for code in (first, second)]
        return first // 32, first % 16, second % 16, dead

    def score(u, slot):
        r, k0, k1, dead = decode(u)
        scores, tops = bank[slot]
        for p in range(4):
            lanes = slice(128 * p, 128 * p + 128)
            keys = jnp.concatenate([k_ref[k0, :, lanes], k_ref[k1, :, lanes]], axis=0)
            s = dot_nn(keys, qd[r, p])
            scores[p] = s
            top = jnp.maximum(
                jnp.max(s[0:128], axis=0, keepdims=True) + dead[0],
                jnp.max(s[128:256], axis=0, keepdims=True) + dead[1],
            )
            tops[p : p + 1, :] = top

    def absorb(u, slot):
        r, k0, k1, dead = decode(u)
        scores, tops = bank[slot]
        before = peaks[r]
        top = jnp.maximum(before, tops[...])
        fade = jnp.exp2(before - top)
        peaks[r] = top
        sums = []
        for p in range(4):
            lanes = slice(128 * p, 128 * p + 128)
            here = top[p : p + 1]
            w0 = jnp.exp2(scores[p, 0:128] - (here - dead[0]))
            w1 = jnp.exp2(scores[p, 128:256] - (here - dead[1]))
            sums.append(jnp.sum(w0, axis=0, keepdims=True) + jnp.sum(w1, axis=0, keepdims=True))
            w = jnp.concatenate([w0.astype(jnp.bfloat16), w1.astype(jnp.bfloat16)], axis=0)
            values = jnp.concatenate([vt_ref[k0, lanes, :], vt_ref[k1, lanes, :]], axis=1)
            o = dot_nn(values, w)
            lo, hi = slice(128 * p, 128 * p + 64), slice(128 * p + 64, 128 * p + 128)
            acc[r, lo, :] = acc[r, lo, :] * fade[p : p + 1, :128] + o[0:64, 0:128]
            acc[r, hi, :] = acc[r, hi, :] * fade[p : p + 1, 128:] + o[64:128, 128:256]
        masses[r] = masses[r] * fade + jnp.concatenate(sums, axis=0)

    score(0, 0)

    def two_units(i, carry):
        u = 2 * i
        score(u + 1, 1)
        absorb(u, 0)
        score(jnp.minimum(u + 2, units), 0)
        absorb(u + 1, 1)
        return carry

    lax.fori_loop(0, (units + 1) // 2, two_units, 0)
    for r in range(NQ):
        mass, peak = masses[r], peaks[r]
        some = mass > 0.0
        safe = jnp.where(some, mass, 1.0)
        inv = jnp.where(some, 1.0 / safe, 0.0)
        lse = jnp.where(some, peak + jnp.log2(safe), LOW)
        for half in range(2):
            found = []
            for p in (2 * half, 2 * half + 1):
                for h in range(2):
                    rows = slice(128 * p + 64 * h, 128 * p + 64 * h + 64)
                    here = slice(128 * (p % 2) + 64 * h, 128 * (p % 2) + 64 * h + 64)
                    side = slice(128 * h, 128 * h + 128)
                    a_ref[r, half, here, :] = (acc[r, rows, :] * inv[p : p + 1, side]).astype(jnp.bfloat16)
                    found.append(lse[p : p + 1, side])
            a_ref[r, half, 256:272, :] = split_lse(jnp.concatenate(found, axis=0))


def attention(sub, q, k, vt):
    vmem = pl.BlockSpec(memory_space=pltpu.VMEM)
    return pl.pallas_call(
        attention_kernel,
        out_shape=pltpu.VMEM((NQ, 2, PACK, 128), jnp.bfloat16),
        in_specs=[pl.BlockSpec(memory_space=pltpu.SMEM), vmem, vmem, vmem],
        out_specs=vmem,
        scratch_shapes=[
            pltpu.SMEM((NQ * NK + 4,), jnp.int32),
            pltpu.VMEM((4, 256, 256), jnp.float32),
            pltpu.VMEM((4, 256, 256), jnp.float32),
            pltpu.VMEM((4, 256), jnp.float32),
            pltpu.VMEM((4, 256), jnp.float32),
            pltpu.VMEM((NQ, 4, 256), jnp.float32),
            pltpu.VMEM((NQ, 4, 256), jnp.float32),
            pltpu.VMEM((NQ, 512, 128), jnp.float32),
        ],
        compiler_params=pltpu.CompilerParams(vmem_limit_bytes=16 * 2**20),
    )(sub, q, k, vt)
class Place:
    def __init__(self):
        row, col = lax.axis_index("row"), lax.axis_index("col")
        self.z, self.y, self.core = row // 2, col // 4, col % 2
        self.x = (row % 2) * 2 + (col // 2) % 2

    def at(self, x=None, y=None, z=None, core=None):
        x = self.x if x is None else x
        y = self.y if y is None else y % 4
        z = self.z if z is None else z % 4
        core = self.core if core is None else core
        return (z * 2 + x // 2, (y * 2 + x % 2) * 2 + core)


def key_blocks(place):
    out = []
    for c in range(2):
        for dx in range(2):
            for dy in range(4):
                x = place.x if dx == 0 else place.x + 1 - 2 * (place.x % 2)
                core = place.core if c == 0 else 1 - place.core
                row, col = place.at(x=x, y=place.y + dy, core=core)
                out.append(row * 16 + col)
    return out


def query_blocks(place):
    out = []
    for dx in range(2):
        for dz in range(4):
            x = place.x if dx == 0 else 3 - place.x
            row, col = place.at(x=x, z=place.z + dz)
            out.append(row * 16 + col)
    return out


class Wire:
    def __init__(self, send_sem, recv_sem):
        self.send_sem, self.recv_sem, self.copies = send_sem, recv_sem, {}

    def send(self, name, src, dst, to):
        m = len(self.copies)
        copy = pltpu.make_async_remote_copy(
            src_ref=src,
            dst_ref=dst,
            send_sem=self.send_sem.at[m],
            recv_sem=self.recv_sem.at[m],
            device_id=to,
            device_id_type=MESH,
        )
        copy.start()
        self.copies[name] = copy

    def arrived(self, name):
        self.copies[name].wait_recv()

    def drain(self):
        for copy in self.copies.values():
            copy.wait_send()


def merged(refs):
    lses = [joined_lse(ref) for ref in refs]
    top = functools.reduce(jnp.maximum, lses)
    parts = [jnp.exp2(lse - top) for lse in lses]
    total = functools.reduce(jnp.add, parts)
    shares = [part / total for part in parts]
    heads = []
    for h in range(4):
        rows = slice(64 * h, 64 * h + 64)
        heads.append(
            functools.reduce(
                jnp.add,
                [ref[rows, :].astype(jnp.float32) * s[h : h + 1, :] for ref, s in zip(refs, shares)],
            )
        )
    return heads, top + jnp.log2(total)


def merge_into(out, refs):
    heads, lse = merged(refs)
    for h in range(4):
        out[64 * h : 64 * h + 64, :] = heads[h].astype(jnp.bfloat16)
    out[256:272, :] = split_lse(lse)


def reduce_and_mix(wire, peers, a, got, mix, x_ref, weights, gain, bias, spare):
    zp, zm, xq = peers
    w_out, w_up, w_down, ready = weights
    slot = lambda dx, dz, h: a.at[dx * 4 + dz, h]
    for h in range(2):
        wire.send(("x2", h), slot(1, 2, h), got.at[h], xq)
    for h in range(2):
        wire.send(("pm", h), slot(1, 1, h), got.at[2 + h], zp)
        wire.send(("mm", h), slot(1, 3, h), got.at[4 + h], zm)
    wire.arrived(("x2", 0))
    merge_into(mix.at[0], [got.at[0], slot(0, 2, 0)])
    wire.send("cp", mix.at[0], got.at[6], zp)
    wire.arrived(("x2", 1))
    merge_into(mix.at[1], [got.at[1], slot(0, 2, 1)])
    wire.send("cm", mix.at[1], got.at[7], zm)
    wire.send(("zp", 1), slot(0, 1, 1), got.at[8], zp)
    wire.send(("zm", 0), slot(0, 3, 0), got.at[9], zm)
    for h in range(2):
        wire.arrived(("pm", h))
        wire.arrived(("mm", h))
        merge_into(mix.at[2 + h], [got.at[2 + h], got.at[4 + h], slot(1, 0, h)])
        wire.send(("x", h), mix.at[2 + h], got.at[10 + h], xq)
    wire.arrived("cp")
    merge_into(mix.at[4], [got.at[6], slot(0, 1, 0)])
    wire.send(("zp", 0), mix.at[4], got.at[12], zp)
    wire.arrived("cm")
    merge_into(mix.at[5], [got.at[7], slot(0, 3, 1)])
    wire.send(("zm", 1), mix.at[5], got.at[13], zm)
    ends = {0: (12, 9, 10), 1: (8, 13, 11)}
    for h in (1, 0):
        for name in (("zp", h), ("zm", h), ("x", h)):
            wire.arrived(name)
        heads, _ = merged([got.at[i] for i in ends[h]] + [slot(0, 0, h)])
        for i in range(4):
            spare[256 * h + 64 * i : 256 * h + 64 * i + 64, :] = heads[i]
    for i in ready:
        i.wait()
    attn = jnp.concatenate(
        [jnp.transpose(spare[128 * i : 128 * i + 128, :]) for i in range(4)], axis=1
    ).astype(jnp.bfloat16)
    mixed = dot_nn(attn, w_out[...])
    hidden = layer_norm(x_ref[...].astype(jnp.float32) + mixed, gain[0:1], bias[0:1]).astype(jnp.bfloat16)
    up = jax.nn.gelu(dot_nn(hidden, w_up[...])).astype(jnp.bfloat16)
    down = dot_nn(up, w_down[...])
    return layer_norm(hidden.astype(jnp.float32) + down, gain[1:2], bias[1:2]).astype(jnp.bfloat16)


def gather_and_project(wire, peers, x_ref, xg, qg, w, wvt, ready, q_ref, k_ref, vt_ref):
    zp, zm, xq, yp, ym, xk, sib = peers

    def part(ref, h):
        return ref.at[pl.ds(HALF * h, HALF)]

    def key(c, dx, dy, h):
        return xg.at[c * 8 + dx * 4 + dy, pl.ds(HALF * h, HALF)]

    def query(dx, dz, h):
        return qg.at[dx * 4 + dz, pl.ds(256 * h, 256)]

    for h in range(2):
        wire.send(("k", 0, 3, h), part(x_ref, h), key(0, 0, 3, h), yp)
        wire.send(("k", 0, 1, 1 - h), part(x_ref, 1 - h), key(0, 0, 1, 1 - h), ym)
        wire.send(("k", 1, 0, h), part(x_ref, h), key(0, 1, 0, h), xk)
    for h in range(2):
        wire.send(("s", 0, 0, h), part(x_ref, h), key(1, 0, 0, h), sib)
    for i in ready:
        i.wait()
    q = dot_nn(x_ref[...], w[:, 0:512]) * (0.125 * LOG2E)
    for i in range(4):
        qg[0, 128 * i : 128 * i + 128, :] = jnp.transpose(q[:, 128 * i : 128 * i + 128]).astype(
            jnp.bfloat16
        )
    for h in range(2):
        wire.send(("q", 0, 3, h), query(0, 0, h), query(0, 3, h), zp)
        wire.send(("q", 0, 1, 1 - h), query(0, 0, 1 - h), query(0, 1, 1 - h), zm)
        wire.send(("q", 1, 0, h), query(0, 0, h), query(1, 0, h), xq)
    wvt[...] = jnp.transpose(w[:, 1024:1536].astype(jnp.float32)).astype(jnp.bfloat16)

    def project(slots):
        rows = jnp.concatenate(
            [x_ref[...] if s == 0 else xg[s] for s in slots], axis=0
        )
        keys = dot_nn(rows, w[:, 512:1024]).astype(jnp.bfloat16)
        values = dot_nt(wvt[...], rows).astype(jnp.bfloat16)
        for i, s in enumerate(slots):
            k_ref[s] = keys[128 * i : 128 * i + 128]
            vt_ref[s] = values[:, 128 * i : 128 * i + 128]

    def spread_query(s):
        for p in range(4):
            q_ref[s, p, 0:64, 0:128] = qg[s, 128 * p : 128 * p + 64, :]
            q_ref[s, p, 64:128, 128:256] = qg[s, 128 * p + 64 : 128 * p + 128, :]

    off = jnp.zeros((64, 128), jnp.bfloat16)
    for s in range(NQ):
        for p in range(4):
            q_ref[s, p, 0:64, 128:256] = off
            q_ref[s, p, 64:128, 0:128] = off

    def across(dx, dy, h):
        wire.send(("s", dx, dy, h), key(0, dx, dy, h), key(1, dx, dy, h), sib)

    wire.arrived(("k", 0, 3, 0))
    wire.send(("k", 0, 2, 0), key(0, 0, 3, 0), key(0, 0, 2, 0), yp)
    across(0, 3, 0)
    wire.arrived(("k", 0, 1, 1))
    wire.send(("k", 0, 2, 1), key(0, 0, 1, 1), key(0, 0, 2, 1), ym)
    across(0, 1, 1)
    wire.arrived(("k", 1, 0, 0))
    wire.send(("k", 1, 3, 0), key(0, 1, 0, 0), key(0, 1, 3, 0), yp)
    wire.send(("k", 1, 1, 0), key(0, 1, 0, 0), key(0, 1, 1, 0), ym)
    across(1, 0, 0)
    wire.arrived(("q", 0, 3, 0))
    wire.send(("q", 0, 2, 0), query(0, 3, 0), query(0, 2, 0), zp)
    wire.arrived(("q", 0, 1, 1))
    wire.send(("q", 0, 2, 1), query(0, 1, 1), query(0, 2, 1), zm)
    wire.arrived(("q", 1, 0, 0))
    wire.send(("q", 1, 3, 0), query(1, 0, 0), query(1, 3, 0), zp)
    wire.send(("q", 1, 1, 0), query(1, 0, 0), query(1, 1, 0), zm)
    wire.arrived(("k", 1, 0, 1))
    wire.send(("k", 1, 3, 1), key(0, 1, 0, 1), key(0, 1, 3, 1), yp)
    wire.send(("k", 1, 1, 1), key(0, 1, 0, 1), key(0, 1, 1, 1), ym)
    across(1, 0, 1)
    wire.arrived(("k", 0, 3, 1))
    across(0, 3, 1)
    wire.arrived(("k", 0, 1, 0))
    across(0, 1, 0)
    for h in range(2):
        wire.arrived(("s", 0, 0, h))
    project((0, 8))
    wire.arrived(("q", 1, 0, 1))
    wire.send(("q", 1, 3, 1), query(1, 0, 1), query(1, 3, 1), zp)
    wire.send(("q", 1, 1, 1), query(1, 0, 1), query(1, 1, 1), zm)
    wire.arrived(("q", 0, 3, 1))
    wire.arrived(("q", 0, 1, 0))
    for h in range(2):
        wire.arrived(("k", 0, 2, h))
        wire.send(("k", 1, 2, h), key(0, 0, 2, h), key(0, 1, 2, h), xk)
        across(0, 2, h)
    project((1, 3))
    for h in range(2):
        wire.arrived(("q", 0, 2, h))
        wire.send(("q", 1, 2, h), query(0, 2, h), query(1, 2, h), xq)
    for dz in range(4):
        spread_query(dz)
    project((2, 4))
    for h in range(2):
        wire.arrived(("k", 1, 3, h))
        across(1, 3, h)
        wire.arrived(("k", 1, 1, h))
        across(1, 1, h)
    for h in range(2):
        for dy in (1, 3):
            wire.arrived(("s", 0, dy, h))
    project((9, 11))
    project((5, 7))
    for h in range(2):
        wire.arrived(("k", 1, 2, h))
        across(1, 2, h)
    for h in range(2):
        wire.arrived(("s", 0, 2, h))
        wire.arrived(("s", 1, 0, h))
    project((10, 12))
    for h in range(2):
        for dy in (1, 3):
            wire.arrived(("s", 1, dy, h))
    project((13, 15))
    for h in range(2):
        wire.arrived(("s", 1, 2, h))
    project((6, 14))
    for dz in (1, 2, 3):
        for h in range(2):
            wire.arrived(("q", 1, dz, h))
    for dz in range(4):
        spread_query(4 + dz)


def link_kernel(layer, reduces, gathers, *refs):
    refs = list(refs)
    x_ref = refs.pop(0)
    starts = not reduces
    if reduces:
        a_ref, w_out_h, w_up_h, w_down_h, gain_ref, bias_ref = refs[:6]
        refs = refs[6:]
    if gathers:
        w_h = refs.pop(0)
    if starts:
        mask_h = refs.pop(0)
    if reduces:
        x_out = refs.pop(0)
    if gathers:
        q_ref, k_ref, vt_ref = refs[:3]
        refs = refs[3:]
    if starts:
        sub_ref = refs.pop(0)
        mask = refs.pop()
    send_sem, recv_sem, copy_sem = refs[:3]
    refs = refs[3:]
    place = Place()
    peers = [
        place.at(z=place.z + 1),
        place.at(z=place.z + 3),
        place.at(x=3 - place.x),
    ]
    if gathers:
        peers += [
            place.at(y=place.y + 1),
            place.at(y=place.y + 3),
            place.at(x=place.x + 1 - 2 * (place.x % 2)),
            place.at(core=1 - place.core),
        ]
    copies = []

    def load(src, dst):
        copy = pltpu.make_async_copy(src, dst, copy_sem.at[len(copies)])
        copy.start()
        copies.append(copy)
        return copy

    if reduces:
        got, mix, spare, w_out, w_up, w_down = refs[:6]
        refs = refs[6:]
        mix_ready = [
            load(w_out_h.at[layer], w_out),
            load(w_up_h.at[layer], w_up),
            load(w_down_h.at[layer], w_down),
        ]
    if gathers:
        xg, qg, w, wvt = refs
        w_ready = [load(w_h.at[layer + 1], w)]
    if starts:
        mask_ready = load(mask_h, mask)
    barrier = pltpu.get_barrier_semaphore()
    for peer in peers:
        pl.semaphore_signal(barrier, inc=1, device_id=peer, device_id_type=MESH)
    pl.semaphore_wait(barrier, len(peers))
    wire = Wire(send_sem, recv_sem)
    if reduces:
        x_out[...] = reduce_and_mix(
            wire, peers[:3], a_ref, got, mix, x_ref, (w_out, w_up, w_down, mix_ready),
            gain_ref[layer], bias_ref[layer], spare,
        )
        x_ref = x_out
    if gathers:
        gather_and_project(wire, peers, x_ref, xg, qg, w, wvt, w_ready, q_ref, k_ref, vt_ref)
    if starts:
        mask_ready.wait()
        queries, keys = query_blocks(place), key_blocks(place)
        for i in range(NQ):
            for j in range(NK):
                sub_ref[i, j] = mask[queries[i], keys[j]]
    wire.drain()


def link(layer, x, reduce_args=None, w_qkv=None, block_mask=None):
    reduces, gathers = reduce_args is not None, w_qkv is not None
    vmem = pl.BlockSpec(memory_space=pltpu.VMEM)
    hbm = pl.BlockSpec(memory_space=pltpu.HBM)
    args, specs, outs = [x], [vmem], []
    scratch = [
        pltpu.SemaphoreType.DMA((14 * reduces + 44 * gathers,)),
        pltpu.SemaphoreType.DMA((14 * reduces + 44 * gathers,)),
        pltpu.SemaphoreType.DMA((4,)),
    ]
    bf16 = jnp.bfloat16
    if reduces:
        args += list(reduce_args)
        specs += [vmem, hbm, hbm, hbm, vmem, vmem]
        outs.append(jax.ShapeDtypeStruct((128, 512), bf16))
        scratch += [
            pltpu.VMEM((14, PACK, 128), bf16),
            pltpu.VMEM((6, PACK, 128), bf16),
            pltpu.VMEM((512, 128), jnp.float32),
            pltpu.VMEM((512, 512), bf16),
            pltpu.VMEM((512, 1024), bf16),
            pltpu.VMEM((1024, 512), bf16),
        ]
    if gathers:
        args.append(w_qkv)
        specs.append(hbm)
        outs += [
            pltpu.VMEM((NQ, 4, 128, 256), bf16),
            pltpu.VMEM((NK, 128, 512), bf16),
            pltpu.VMEM((NK, 512, 128), bf16),
        ]
        scratch += [
            pltpu.VMEM((NK, 128, 512), bf16),
            pltpu.VMEM((NQ, 512, 128), bf16),
            pltpu.VMEM((512, 1536), bf16),
            pltpu.VMEM((512, 512), bf16),
        ]
    out_specs = [vmem for _ in outs]
    if not reduces:
        args.append(block_mask)
        specs.append(hbm)
        outs.append(jax.ShapeDtypeStruct((NQ, NK), jnp.int32))
        out_specs.append(pl.BlockSpec(memory_space=pltpu.SMEM))
        scratch.append(pltpu.SMEM((128, 128), jnp.int32))
    return pl.pallas_call(
        functools.partial(link_kernel, layer, reduces, gathers),
        out_shape=tuple(outs),
        in_specs=specs,
        out_specs=tuple(out_specs),
        scratch_shapes=scratch,
        compiler_params=pltpu.CompilerParams(
            collective_id=layer + 1, has_side_effects=True, vmem_limit_bytes=24 * 2**20
        ),
    )(*args)


def per_device(node_feats, block_mask, w_qkv, w_out, w_up, w_down, ln_gain, ln_bias):
    x = node_feats
    q, k, vt, sub = link(-1, x, w_qkv=w_qkv, block_mask=block_mask)
    for layer in range(LAYERS):
        parts = attention(sub, q, k, vt)
        last = layer == LAYERS - 1
        rest = (parts, w_out, w_up, w_down, ln_gain, ln_bias)
        if last:
            (x,) = link(layer, x, reduce_args=rest)
        else:
            x, q, k, vt = link(layer, x, reduce_args=rest, w_qkv=w_qkv)
    return x


def solution(mesh):
    placed = (P(("row", "col"), None), P(), P(), P(), P(), P(), P(), P())
    return jax.shard_map(
        per_device, mesh=mesh, in_specs=placed, out_specs=P(("row", "col"), None), check_vma=False
    )
```

```python
import functools

import jax
import jax.numpy as jnp
from jax import lax
from jax.experimental import pallas as pl
from jax.experimental.pallas import tpu as pltpu
from jax.sharding import PartitionSpec as P

HEADS = 8
BLOCK = 128
LAYERS = 2
NQ = 8
NK = 16
LOG2E = 1.4426950408889634
LOW = -1e30
PACK = 144
PLUS, MINUS = (0, 1), (2, 3)
MESH = pl.DeviceIdType.MESH


def dot_nn(a, b):
    return lax.dot_general(a, b, (((1,), (0,)), ((), ())), preferred_element_type=jnp.float32)


def dot_nt(a, b):
    return lax.dot_general(a, b, (((1,), (1,)), ((), ())), preferred_element_type=jnp.float32)


def layer_norm(values, gain, bias):
    center = values - jnp.mean(values, axis=-1, keepdims=True)
    spread = jnp.mean(center * center, axis=-1, keepdims=True)
    return center * lax.rsqrt(spread + 1e-05) * gain + bias


def split_lse(lse):
    high = lse.astype(jnp.bfloat16).astype(jnp.float32)
    rest = lse - high
    mid = rest.astype(jnp.bfloat16).astype(jnp.float32)
    low = rest - mid
    pad = jnp.zeros((10, 128), jnp.float32)
    return jnp.concatenate([high, mid, low, pad], axis=0).astype(jnp.bfloat16)


def joined_lse(ref):
    parts = ref[128:PACK, :].astype(jnp.float32)
    return parts[0:2] + parts[2:4] + parts[4:6]


def attention_kernel(sub_ref, qd, k_ref, vt_ref, a_ref, order, scores_a, scores_b, tops_a, tops_b, peaks, masses, acc):
    bank = ((scores_a, tops_a), (scores_b, tops_b))
    count = jnp.int32(0)
    for r in range(NQ):
        for k in range(NK):
            order[count] = 32 * r + k
            count = count + sub_ref[r, k]
        order[count] = order[jnp.maximum(count - 1, 0)] + 16
        count = count + count % 2
    units = count // 2
    last = jnp.maximum(count - 1, 0)
    tail = order[last]
    order[count] = tail - tail % 32 + tail % 16 + 16
    order[count + 1] = order[count]
    peaks[...] = jnp.full_like(peaks, LOW)
    masses[...] = jnp.zeros_like(masses)
    acc[...] = jnp.zeros_like(acc)

    def decode(u):
        first, second = order[2 * u], order[2 * u + 1]
        dead = [jnp.where((code // 16) % 2 == 1, LOW, 0.0) for code in (first, second)]
        return first // 32, first % 16, second % 16, dead

    def score(u, slot):
        r, k0, k1, dead = decode(u)
        scores, tops = bank[slot]
        for p in range(4):
            lanes = slice(128 * p, 128 * p + 128)
            keys = jnp.concatenate([k_ref[k0, :, lanes], k_ref[k1, :, lanes]], axis=0)
            s = dot_nn(keys, qd[r, p])
            scores[p] = s
            top = jnp.maximum(
                jnp.max(s[0:128], axis=0, keepdims=True) + dead[0],
                jnp.max(s[128:256], axis=0, keepdims=True) + dead[1],
            )
            tops[p : p + 1, :] = top

    def absorb(u, slot):
        r, k0, k1, dead = decode(u)
        scores, tops = bank[slot]
        before = peaks[r]
        top = jnp.maximum(before, tops[...])
        fade = jnp.exp2(before - top)
        peaks[r] = top
        sums = []
        for p in range(4):
            lanes = slice(128 * p, 128 * p + 128)
            here = top[p : p + 1]
            w0 = jnp.exp2(scores[p, 0:128] - (here - dead[0]))
            w1 = jnp.exp2(scores[p, 128:256] - (here - dead[1]))
            sums.append(jnp.sum(w0, axis=0, keepdims=True) + jnp.sum(w1, axis=0, keepdims=True))
            w = jnp.concatenate([w0.astype(jnp.bfloat16), w1.astype(jnp.bfloat16)], axis=0)
            values = jnp.concatenate([vt_ref[k0, lanes, :], vt_ref[k1, lanes, :]], axis=1)
            o = dot_nn(values, w)
            lo, hi = slice(128 * p, 128 * p + 64), slice(128 * p + 64, 128 * p + 128)
            acc[r, lo, :] = acc[r, lo, :] * fade[p : p + 1, :128] + o[0:64, 0:128]
            acc[r, hi, :] = acc[r, hi, :] * fade[p : p + 1, 128:] + o[64:128, 128:256]
        masses[r] = masses[r] * fade + jnp.concatenate(sums, axis=0)

    score(0, 0)

    def two_units(i, carry):
        u = 2 * i
        score(u + 1, 1)
        absorb(u, 0)
        score(jnp.minimum(u + 2, units), 0)
        absorb(u + 1, 1)
        return carry

    lax.fori_loop(0, (units + 1) // 2, two_units, 0)
    for r in range(NQ):
        mass, peak = masses[r], peaks[r]
        some = mass > 0.0
        safe = jnp.where(some, mass, 1.0)
        inv = jnp.where(some, 1.0 / safe, 0.0)
        lse = jnp.where(some, peak + jnp.log2(safe), LOW)
        for p in range(4):
            for h in range(2):
                rows = slice(128 * p + 64 * h, 128 * p + 64 * h + 64)
                side = slice(128 * h, 128 * h + 128)
                a_ref[r, p, 64 * h : 64 * h + 64, :] = (
                    acc[r, rows, :] * inv[p : p + 1, side]
                ).astype(jnp.bfloat16)
            pair = jnp.concatenate([lse[p : p + 1, :128], lse[p : p + 1, 128:]], axis=0)
            a_ref[r, p, 128:PACK, :] = split_lse(pair)


def attention(sub, q, k, vt):
    vmem = pl.BlockSpec(memory_space=pltpu.VMEM)
    return pl.pallas_call(
        attention_kernel,
        out_shape=pltpu.VMEM((NQ, 4, PACK, 128), jnp.bfloat16),
        in_specs=[pl.BlockSpec(memory_space=pltpu.SMEM), vmem, vmem, vmem],
        out_specs=vmem,
        scratch_shapes=[
            pltpu.SMEM((NQ * NK + 4,), jnp.int32),
            pltpu.VMEM((4, 256, 256), jnp.float32),
            pltpu.VMEM((4, 256, 256), jnp.float32),
            pltpu.VMEM((4, 256), jnp.float32),
            pltpu.VMEM((4, 256), jnp.float32),
            pltpu.VMEM((NQ, 4, 256), jnp.float32),
            pltpu.VMEM((NQ, 4, 256), jnp.float32),
            pltpu.VMEM((NQ, 512, 128), jnp.float32),
        ],
        compiler_params=pltpu.CompilerParams(vmem_limit_bytes=16 * 2**20),
    )(sub, q, k, vt)
class Place:
    def __init__(self):
        row, col = lax.axis_index("row"), lax.axis_index("col")
        self.z, self.y, self.core = row // 2, col // 4, col % 2
        self.x = (row % 2) * 2 + (col // 2) % 2

    def at(self, x=None, y=None, z=None, core=None):
        x = self.x if x is None else x
        y = self.y if y is None else y % 4
        z = self.z if z is None else z % 4
        core = self.core if core is None else core
        return (z * 2 + x // 2, (y * 2 + x % 2) * 2 + core)


def key_blocks(place):
    out = []
    for c in range(2):
        for dx in range(2):
            for dy in range(4):
                x = place.x if dx == 0 else place.x + 1 - 2 * (place.x % 2)
                core = place.core if c == 0 else 1 - place.core
                row, col = place.at(x=x, y=place.y + dy, core=core)
                out.append(row * 16 + col)
    return out


def query_blocks(place):
    out = []
    for dx in range(2):
        for dz in range(4):
            x = place.x if dx == 0 else 3 - place.x
            row, col = place.at(x=x, z=place.z + dz)
            out.append(row * 16 + col)
    return out


class Wire:
    def __init__(self, send_sem, recv_sem):
        self.send_sem, self.recv_sem, self.copies = send_sem, recv_sem, {}

    def send(self, name, src, dst, to):
        m = len(self.copies)
        copy = pltpu.make_async_remote_copy(
            src_ref=src,
            dst_ref=dst,
            send_sem=self.send_sem.at[m],
            recv_sem=self.recv_sem.at[m],
            device_id=to,
            device_id_type=MESH,
        )
        copy.start()
        self.copies[name] = copy

    def arrived(self, name):
        self.copies[name].wait_recv()

    def drain(self):
        for copy in self.copies.values():
            copy.wait_send()


def merged(refs):
    lses = [joined_lse(ref) for ref in refs]
    top = functools.reduce(jnp.maximum, lses)
    parts = [jnp.exp2(lse - top) for lse in lses]
    total = functools.reduce(jnp.add, parts)
    shares = [part / total for part in parts]
    heads = []
    for h in range(2):
        rows = slice(64 * h, 64 * h + 64)
        heads.append(
            functools.reduce(
                jnp.add,
                [ref[rows, :].astype(jnp.float32) * s[h : h + 1, :] for ref, s in zip(refs, shares)],
            )
        )
    return jnp.concatenate(heads, axis=0), top + jnp.log2(total)


def merge_into(out, refs):
    both, lse = merged(refs)
    out[0:128, :] = both.astype(jnp.bfloat16)
    out[128:PACK, :] = split_lse(lse)


def reduce_and_mix(wire, peers, a, got, mix, x_ref, weights, gain, bias):
    zp, zm, xq = peers
    w_out, w_up, w_down, ready = weights

    def slot(dx, dz, j, n=1):
        return a.at[dx * 4 + dz, pl.ds(j, n)] if n > 1 else a.at[dx * 4 + dz, j]

    def run(ref, j, n=1):
        return ref.at[pl.ds(j, n)] if n > 1 else ref.at[j]

    for j in (0, 2, 1, 3):
        wire.send(("x2", j), slot(1, 2, j), run(got, j), xq)
    for h in range(2):
        wire.send(("pm", h), slot(1, 1, 2 * h, 2), run(got, 4 + 2 * h, 2), zp)
        wire.send(("mm", h), slot(1, 3, 2 * h, 2), run(got, 8 + 2 * h, 2), zm)
    for j in (0, 2, 1, 3):
        wire.arrived(("x2", j))
        merge_into(run(mix, j), [run(got, j), slot(0, 2, j)])
        wire.send(("c", j), run(mix, j), run(got, 12 + j), zp if j in PLUS else zm)
    wire.send("zp", slot(0, 1, 2, 2), run(got, 18, 2), zp)
    wire.send("zm", slot(0, 3, 0, 2), run(got, 20, 2), zm)
    for h in range(2):
        wire.arrived(("pm", h))
        wire.arrived(("mm", h))
        for j in (2 * h, 2 * h + 1):
            merge_into(run(mix, 4 + j), [run(got, 4 + j), run(got, 8 + j), slot(1, 0, j)])
        wire.send(("x", h), run(mix, 4 + 2 * h, 2), run(got, 24 + 2 * h, 2), xq)
    for j in (0, 2, 1, 3):
        wire.arrived(("c", j))
        if j in PLUS:
            merge_into(run(mix, 8 + j), [run(got, 12 + j), slot(0, 1, j)])
            wire.send(("z", j), run(mix, 8 + j), run(got, 16 + j), zp)
        else:
            merge_into(run(mix, 8 + j), [run(got, 12 + j), slot(0, 3, j)])
            wire.send(("z", j), run(mix, 8 + j), run(got, 20 + j), zm)
    for i in ready:
        i.wait()
    mixed = x_ref[...].astype(jnp.float32)
    wire.arrived("zp")
    wire.arrived("zm")
    wire.arrived(("x", 0))
    wire.arrived(("x", 1))
    for j in (0, 2, 1, 3):
        wire.arrived(("z", j))
        both, _ = merged([run(got, 16 + j), run(got, 20 + j), run(got, 24 + j), slot(0, 0, j)])
        attn = jnp.transpose(both).astype(jnp.bfloat16)
        mixed = mixed + dot_nn(attn, w_out[128 * j : 128 * j + 128, :])
    hidden = layer_norm(mixed, gain[0:1], bias[0:1]).astype(jnp.bfloat16)
    up = jax.nn.gelu(dot_nn(hidden, w_up[...])).astype(jnp.bfloat16)
    down = dot_nn(up, w_down[...])
    return layer_norm(hidden.astype(jnp.float32) + down, gain[1:2], bias[1:2]).astype(jnp.bfloat16)


def gather_and_project(wire, peers, x_ref, xg, qg, w, wvt, ready, q_ref, k_ref, vt_ref):
    zp, zm, xq, yp, ym, xk, sib = peers

    def part(ref, j, n=1):
        return ref.at[pl.ds(32 * j, 32 * n)]

    def key(c, dx, dy, j=0, n=4):
        return xg.at[c * 8 + dx * 4 + dy, pl.ds(32 * j, 32 * n)]

    def query(dx, dz, j=0, n=4):
        return qg.at[dx * 4 + dz, pl.ds(128 * j, 128 * n)]

    def across(dx, dy, j=0, n=4):
        wire.send(("s", dx, dy, j), key(0, dx, dy, j, n), key(1, dx, dy, j, n), sib)

    for i in range(4):
        j = (i + 2) % 4
        wire.send(("k", 0, 3, i), part(x_ref, i), key(0, 0, 3, i, 1), yp)
        wire.send(("k", 0, 1, j), part(x_ref, j), key(0, 0, 1, j, 1), ym)
        if i % 2 == 0:
            wire.send(("k", 1, 0, i), part(x_ref, i, 2), key(0, 1, 0, i, 2), xk)
    wire.send(("s", 0, 0, 0), part(x_ref, 0, 4), key(1, 0, 0), sib)
    for i in ready:
        i.wait()
    q = dot_nn(x_ref[...], w[:, 0:512]) * (0.125 * LOG2E)
    for i in range(4):
        qg[0, 128 * i : 128 * i + 128, :] = jnp.transpose(q[:, 128 * i : 128 * i + 128]).astype(
            jnp.bfloat16
        )
    for i in range(4):
        j = (i + 2) % 4
        wire.send(("q", 0, 3, i), query(0, 0, i, 1), query(0, 3, i, 1), zp)
        wire.send(("q", 0, 1, j), query(0, 0, j, 1), query(0, 1, j, 1), zm)
        if i % 2 == 0:
            wire.send(("q", 1, 0, i), query(0, 0, i, 2), query(1, 0, i, 2), xq)
    wvt[...] = jnp.transpose(w[:, 1024:1536].astype(jnp.float32)).astype(jnp.bfloat16)
    off = jnp.zeros((64, 128), jnp.bfloat16)
    for s in range(NQ):
        for p in range(4):
            q_ref[s, p, 0:64, 128:256] = off
            q_ref[s, p, 64:128, 0:128] = off

    def project(slots):
        rows = jnp.concatenate([x_ref[...] if s == 0 else xg[s] for s in slots], axis=0)
        keys = dot_nn(rows, w[:, 512:1024]).astype(jnp.bfloat16)
        values = dot_nt(wvt[...], rows).astype(jnp.bfloat16)
        for i, s in enumerate(slots):
            k_ref[s] = keys[128 * i : 128 * i + 128]
            vt_ref[s] = values[:, 128 * i : 128 * i + 128]

    def spread_query(s):
        for p in range(4):
            q_ref[s, p, 0:64, 0:128] = qg[s, 128 * p : 128 * p + 64, :]
            q_ref[s, p, 64:128, 128:256] = qg[s, 128 * p + 64 : 128 * p + 128, :]

    for i in range(2):
        wire.arrived(("k", 0, 3, i))
        wire.send(("k", 0, 2, i), key(0, 0, 3, i, 1), key(0, 0, 2, i, 1), yp)
        wire.arrived(("k", 0, 1, 2 + i))
        wire.send(("k", 0, 2, 2 + i), key(0, 0, 1, 2 + i, 1), key(0, 0, 2, 2 + i, 1), ym)
    for i in range(2):
        wire.arrived(("q", 0, 3, i))
        wire.send(("q", 0, 2, i), query(0, 3, i, 1), query(0, 2, i, 1), zp)
        wire.arrived(("q", 0, 1, 2 + i))
        wire.send(("q", 0, 2, 2 + i), query(0, 1, 2 + i, 1), query(0, 2, 2 + i, 1), zm)
    for i in (0, 2):
        wire.arrived(("k", 1, 0, i))
        wire.send(("k", 1, 3, i), key(0, 1, 0, i, 2), key(0, 1, 3, i, 2), yp)
        wire.send(("k", 1, 1, i), key(0, 1, 0, i, 2), key(0, 1, 1, i, 2), ym)
        wire.arrived(("q", 1, 0, i))
        wire.send(("q", 1, 3, i), query(1, 0, i, 2), query(1, 3, i, 2), zp)
        wire.send(("q", 1, 1, i), query(1, 0, i, 2), query(1, 1, i, 2), zm)
    across(1, 0)
    for i in range(2):
        wire.arrived(("k", 0, 3, 2 + i))
        wire.arrived(("k", 0, 1, i))
    across(0, 3)
    across(0, 1)
    wire.arrived(("s", 0, 0, 0))
    project((0, 8))
    for j in (0, 2, 1, 3):
        wire.arrived(("k", 0, 2, j))
        wire.send(("k", 1, 2, j), key(0, 0, 2, j, 1), key(0, 1, 2, j, 1), xk)
    across(0, 2)
    for j in (0, 2, 1, 3):
        wire.arrived(("q", 0, 2, j))
        wire.send(("q", 1, 2, j), query(0, 2, j, 1), query(1, 2, j, 1), xq)
    project((1, 3))
    project((2, 4))
    for i in range(2):
        wire.arrived(("q", 0, 3, 2 + i))
        wire.arrived(("q", 0, 1, i))
    for dz in range(4):
        spread_query(dz)
    for dx, dy in ((1, 0), (0, 3), (0, 1), (0, 2)):
        wire.arrived(("s", dx, dy, 0))
    project((9, 11))
    for i in (0, 2):
        for dy in (1, 3):
            wire.arrived(("k", 1, dy, i))
            across(1, dy, i, 2)
    project((10, 12))
    for j in (0, 2, 1, 3):
        wire.arrived(("k", 1, 2, j))
        across(1, 2, j, 1)
    project((5, 7))
    for i in (0, 2):
        for dy in (1, 3):
            wire.arrived(("s", 1, dy, i))
    project((13, 15))
    for j in (0, 2, 1, 3):
        wire.arrived(("s", 1, 2, j))
    project((6, 14))
    for i in (0, 2):
        for dz in (1, 3):
            wire.arrived(("q", 1, dz, i))
    for j in range(4):
        wire.arrived(("q", 1, 2, j))
    for dz in range(4):
        spread_query(4 + dz)


def link_kernel(layer, reduces, gathers, *refs):
    refs = list(refs)
    x_ref = refs.pop(0)
    starts = not reduces
    if reduces:
        a_ref, w_out_h, w_up_h, w_down_h, gain_ref, bias_ref = refs[:6]
        refs = refs[6:]
    if gathers:
        w_h = refs.pop(0)
    if starts:
        mask_h = refs.pop(0)
    if reduces:
        x_out = refs.pop(0)
    if gathers:
        q_ref, k_ref, vt_ref = refs[:3]
        refs = refs[3:]
    if starts:
        sub_ref = refs.pop(0)
        mask, x_own = refs[-2:]
        refs = refs[:-2]
    send_sem, recv_sem, copy_sem = refs[:3]
    refs = refs[3:]
    place = Place()
    peers = [
        place.at(z=place.z + 1),
        place.at(z=place.z + 3),
        place.at(x=3 - place.x),
    ]
    if gathers:
        peers += [
            place.at(y=place.y + 1),
            place.at(y=place.y + 3),
            place.at(x=place.x + 1 - 2 * (place.x % 2)),
            place.at(core=1 - place.core),
        ]
    copies = []

    def load(src, dst):
        copy = pltpu.make_async_copy(src, dst, copy_sem.at[len(copies)])
        copy.start()
        copies.append(copy)
        return copy

    if starts:
        x_ready = load(x_ref, x_own)
        x_ref = x_own
    if reduces:
        got, mix, w_out, w_up, w_down = refs[:5]
        refs = refs[5:]
        mix_ready = [
            load(w_out_h.at[layer], w_out),
            load(w_up_h.at[layer], w_up),
            load(w_down_h.at[layer], w_down),
        ]
    if gathers:
        xg, qg, w, wvt = refs
        w_ready = [load(w_h.at[layer + 1], w)]
    if starts:
        mask_ready = load(mask_h, mask)
    barrier = pltpu.get_barrier_semaphore()
    for peer in peers:
        pl.semaphore_signal(barrier, inc=1, device_id=peer, device_id_type=MESH)
    pl.semaphore_wait(barrier, len(peers))
    wire = Wire(send_sem, recv_sem)
    if starts:
        x_ready.wait()
    if reduces:
        x_out[...] = reduce_and_mix(
            wire, peers[:3], a_ref, got, mix, x_ref, (w_out, w_up, w_down, mix_ready),
            gain_ref[layer], bias_ref[layer],
        )
        x_ref = x_out
    if gathers:
        gather_and_project(wire, peers, x_ref, xg, qg, w, wvt, w_ready, q_ref, k_ref, vt_ref)
    if starts:
        mask_ready.wait()
        queries, keys = query_blocks(place), key_blocks(place)
        for i in range(NQ):
            for j in range(NK):
                sub_ref[i, j] = mask[queries[i], keys[j]]
    wire.drain()


def link(layer, x, reduce_args=None, w_qkv=None, block_mask=None):
    reduces, gathers = reduce_args is not None, w_qkv is not None
    vmem = pl.BlockSpec(memory_space=pltpu.VMEM)
    hbm = pl.BlockSpec(memory_space=pltpu.HBM)
    args, specs, outs = [x], [vmem if reduces else hbm], []
    scratch = [
        pltpu.SemaphoreType.DMA((20 * reduces + 57 * gathers,)),
        pltpu.SemaphoreType.DMA((20 * reduces + 57 * gathers,)),
        pltpu.SemaphoreType.DMA((4,)),
    ]
    bf16 = jnp.bfloat16
    if reduces:
        args += list(reduce_args)
        specs += [vmem, hbm, hbm, hbm, vmem, vmem]
        outs.append(jax.ShapeDtypeStruct((128, 512), bf16))
        scratch += [
            pltpu.VMEM((28, PACK, 128), bf16),
            pltpu.VMEM((12, PACK, 128), bf16),
            pltpu.VMEM((512, 512), bf16),
            pltpu.VMEM((512, 1024), bf16),
            pltpu.VMEM((1024, 512), bf16),
        ]
    if gathers:
        args.append(w_qkv)
        specs.append(hbm)
        outs += [
            pltpu.VMEM((NQ, 4, 128, 256), bf16),
            pltpu.VMEM((NK, 128, 512), bf16),
            pltpu.VMEM((NK, 512, 128), bf16),
        ]
        scratch += [
            pltpu.VMEM((NK, 128, 512), bf16),
            pltpu.VMEM((NQ, 512, 128), bf16),
            pltpu.VMEM((512, 1536), bf16),
            pltpu.VMEM((512, 512), bf16),
        ]
    out_specs = [vmem for _ in outs]
    if not reduces:
        args.append(block_mask)
        specs.append(hbm)
        outs.append(jax.ShapeDtypeStruct((NQ, NK), jnp.int32))
        out_specs.append(pl.BlockSpec(memory_space=pltpu.SMEM))
        scratch += [pltpu.SMEM((128, 128), jnp.int32), pltpu.VMEM((128, 512), bf16)]
    return pl.pallas_call(
        functools.partial(link_kernel, layer, reduces, gathers),
        out_shape=tuple(outs),
        in_specs=specs,
        out_specs=tuple(out_specs),
        scratch_shapes=scratch,
        compiler_params=pltpu.CompilerParams(
            collective_id=layer + 1, has_side_effects=True, vmem_limit_bytes=24 * 2**20
        ),
    )(*args)


def per_device(node_feats, block_mask, w_qkv, w_out, w_up, w_down, ln_gain, ln_bias):
    x = node_feats
    w_qkv, w_out, w_up, w_down, block_mask = (
        pltpu.with_memory_space_constraint(a, pltpu.HBM)
        for a in (w_qkv, w_out, w_up, w_down, block_mask)
    )
    x_first = pltpu.with_memory_space_constraint(x, pltpu.HBM)
    q, k, vt, sub = link(-1, x_first, w_qkv=w_qkv, block_mask=block_mask)
    for layer in range(LAYERS):
        parts = attention(sub, q, k, vt)
        last = layer == LAYERS - 1
        rest = (parts, w_out, w_up, w_down, ln_gain, ln_bias)
        if last:
            (x,) = link(layer, x, reduce_args=rest)
        else:
            x, q, k, vt = link(layer, x, reduce_args=rest, w_qkv=w_qkv)
    return x


def solution(mesh):
    placed = (P(("row", "col"), None), P(), P(), P(), P(), P(), P(), P())
    return jax.shard_map(
        per_device, mesh=mesh, in_specs=placed, out_specs=P(("row", "col"), None), check_vma=False
    )
```

```python
import functools

import jax
import jax.numpy as jnp
from jax import lax
from jax.experimental import pallas as pl
from jax.experimental.pallas import tpu as pltpu
from jax.sharding import PartitionSpec as P

HEADS = 8
BLOCK = 128
LAYERS = 2
NQ = 8
NK = 16
LOG2E = 1.4426950408889634
LOW = -1e30
PACK = 144
PLUS, MINUS = (0, 1), (2, 3)
MESH = pl.DeviceIdType.MESH


def dot_nn(a, b):
    return lax.dot_general(a, b, (((1,), (0,)), ((), ())), preferred_element_type=jnp.float32)


def dot_nt(a, b):
    return lax.dot_general(a, b, (((1,), (1,)), ((), ())), preferred_element_type=jnp.float32)


def layer_norm(values, gain, bias):
    center = values - jnp.mean(values, axis=-1, keepdims=True)
    spread = jnp.mean(center * center, axis=-1, keepdims=True)
    return center * lax.rsqrt(spread + 1e-05) * gain + bias


def split_lse(lse):
    high = lse.astype(jnp.bfloat16).astype(jnp.float32)
    rest = lse - high
    mid = rest.astype(jnp.bfloat16).astype(jnp.float32)
    low = rest - mid
    pad = jnp.zeros((10, 128), jnp.float32)
    return jnp.concatenate([high, mid, low, pad], axis=0).astype(jnp.bfloat16)


def joined_lse(ref):
    parts = ref[128:PACK, :].astype(jnp.float32)
    return parts[0:2] + parts[2:4] + parts[4:6]


def finish_parts(peaks, masses, acc, a_ref):
    for r in range(NQ):
        mass, peak = masses[r], peaks[r]
        some = mass > 0.0
        safe = jnp.where(some, mass, 1.0)
        inv = jnp.where(some, 1.0 / safe, 0.0)
        lse = jnp.where(some, peak + jnp.log2(safe), LOW)
        for p in range(4):
            for h in range(2):
                rows = slice(128 * p + 64 * h, 128 * p + 64 * h + 64)
                side = slice(128 * h, 128 * h + 128)
                a_ref[r, p, 64 * h : 64 * h + 64, :] = (
                    acc[r, rows, :] * inv[p : p + 1, side]
                ).astype(jnp.bfloat16)
            pair = jnp.concatenate([lse[p : p + 1, :128], lse[p : p + 1, 128:]], axis=0)
            a_ref[r, p, 128:PACK, :] = split_lse(pair)


def attention_kernel(
    sub_any, qd, k_ref, vt_ref, peaks, masses, acc,
    sub_ref, sub_sem, order, scores_a, scores_b, tops_a, tops_b,
):
    sub_copy = pltpu.make_async_copy(sub_any, sub_ref, sub_sem)
    sub_copy.start()
    peaks[...] = jnp.full_like(peaks, LOW)
    masses[...] = jnp.zeros_like(masses)
    acc[...] = jnp.zeros_like(acc)
    sub_copy.wait()
    bank = ((scores_a, tops_a), (scores_b, tops_b))
    count = jnp.int32(0)
    for r in range(NQ):
        for k in range(NK):
            order[count] = 32 * r + k
            count = count + sub_ref[r, k]
        order[count] = order[jnp.maximum(count - 1, 0)] + 16
        count = count + count % 2
    units = count // 2
    last = jnp.maximum(count - 1, 0)
    tail = order[last]
    order[count] = tail - tail % 32 + tail % 16 + 16
    order[count + 1] = order[count]

    def decode(u):
        first, second = order[2 * u], order[2 * u + 1]
        dead = [jnp.where((code // 16) % 2 == 1, LOW, 0.0) for code in (first, second)]
        return first // 32, first % 16, second % 16, dead

    def score(u, slot, p):
        r, k0, k1, dead = decode(u)
        scores, tops = bank[slot]
        lanes = slice(128 * p, 128 * p + 128)
        keys = jnp.concatenate([k_ref[k0, :, lanes], k_ref[k1, :, lanes]], axis=0)
        s = dot_nn(keys, qd[r, p])
        scores[p] = s
        top = jnp.maximum(
            jnp.max(s[0:128], axis=0, keepdims=True) + dead[0],
            jnp.max(s[128:256], axis=0, keepdims=True) + dead[1],
        )
        tops[p : p + 1, :] = top

    def absorb(u, slot, p):
        r, k0, k1, dead = decode(u)
        scores, tops = bank[slot]
        before = peaks[r, p : p + 1, :]
        here = jnp.maximum(before, tops[p : p + 1, :])
        fade = jnp.exp2(before - here)
        peaks[r, p : p + 1, :] = here
        lanes = slice(128 * p, 128 * p + 128)
        w0 = jnp.exp2(scores[p, 0:128] - (here - dead[0]))
        w1 = jnp.exp2(scores[p, 128:256] - (here - dead[1]))
        mass = jnp.sum(w0, axis=0, keepdims=True) + jnp.sum(w1, axis=0, keepdims=True)
        w = jnp.concatenate([w0.astype(jnp.bfloat16), w1.astype(jnp.bfloat16)], axis=0)
        values = jnp.concatenate([vt_ref[k0, lanes, :], vt_ref[k1, lanes, :]], axis=1)
        o = dot_nn(values, w)
        lo, hi = slice(128 * p, 128 * p + 64), slice(128 * p + 64, 128 * p + 128)
        acc[r, lo, :] = acc[r, lo, :] * fade[:, :128] + o[0:64, 0:128]
        acc[r, hi, :] = acc[r, hi, :] * fade[:, 128:] + o[64:128, 128:256]
        masses[r, p : p + 1, :] = masses[r, p : p + 1, :] * fade + mass

    for p in range(4):
        score(0, 0, p)

    def two_units(i, carry):
        u = 2 * i
        for p in range(4):
            score(u + 1, 1, p)
            absorb(u, 0, p)
        for p in range(4):
            score(jnp.minimum(u + 2, units), 0, p)
            absorb(u + 1, 1, p)
        return carry

    lax.fori_loop(0, (units + 1) // 2, two_units, 0)


def attention(sub, q, k, vt):
    vmem = pl.BlockSpec(memory_space=pltpu.VMEM)
    return pl.pallas_call(
        attention_kernel,
        out_shape=(
            pltpu.VMEM((NQ, 4, 256), jnp.float32),
            pltpu.VMEM((NQ, 4, 256), jnp.float32),
            pltpu.VMEM((NQ, 512, 128), jnp.float32),
        ),
        in_specs=[pl.BlockSpec(memory_space=pl.ANY), vmem, vmem, vmem],
        out_specs=(vmem, vmem, vmem),
        scratch_shapes=[
            pltpu.SMEM((NQ, NK), jnp.int32),
            pltpu.SemaphoreType.DMA,
            pltpu.SMEM((NQ * NK + 4,), jnp.int32),
            pltpu.VMEM((4, 256, 256), jnp.float32),
            pltpu.VMEM((4, 256, 256), jnp.float32),
            pltpu.VMEM((4, 256), jnp.float32),
            pltpu.VMEM((4, 256), jnp.float32),
        ],
        compiler_params=pltpu.CompilerParams(vmem_limit_bytes=16 * 2**20),
    )(sub, q, k, vt)


class Place:
    def __init__(self):
        row, col = lax.axis_index("row"), lax.axis_index("col")
        self.z, self.y, self.core = row // 2, col // 4, col % 2
        self.x = (row % 2) * 2 + (col // 2) % 2

    def at(self, x=None, y=None, z=None, core=None):
        x = self.x if x is None else x
        y = self.y if y is None else y % 4
        z = self.z if z is None else z % 4
        core = self.core if core is None else core
        return (z * 2 + x // 2, (y * 2 + x % 2) * 2 + core)


def key_blocks(place):
    out = []
    for c in range(2):
        for dx in range(2):
            for dy in range(4):
                x = place.x if dx == 0 else place.x + 1 - 2 * (place.x % 2)
                core = place.core if c == 0 else 1 - place.core
                row, col = place.at(x=x, y=place.y + dy, core=core)
                out.append(row * 16 + col)
    return out


def query_blocks(place):
    out = []
    for dx in range(2):
        for dz in range(4):
            x = place.x if dx == 0 else 3 - place.x
            row, col = place.at(x=x, z=place.z + dz)
            out.append(row * 16 + col)
    return out


class Wire:
    def __init__(self, send_sem, recv_sem):
        self.send_sem, self.recv_sem, self.copies = send_sem, recv_sem, {}

    def send(self, name, src, dst, to):
        m = len(self.copies)
        copy = pltpu.make_async_remote_copy(
            src_ref=src,
            dst_ref=dst,
            send_sem=self.send_sem.at[m],
            recv_sem=self.recv_sem.at[m],
            device_id=to,
            device_id_type=MESH,
        )
        copy.start()
        self.copies[name] = copy

    def arrived(self, name):
        self.copies[name].wait_recv()

    def drain(self):
        for copy in self.copies.values():
            copy.wait_send()


def merged(refs):
    lses = [joined_lse(ref) for ref in refs]
    top = functools.reduce(jnp.maximum, lses)
    parts = [jnp.exp2(lse - top) for lse in lses]
    total = functools.reduce(jnp.add, parts)
    shares = [part / total for part in parts]
    heads = []
    for h in range(2):
        rows = slice(64 * h, 64 * h + 64)
        heads.append(
            functools.reduce(
                jnp.add,
                [ref[rows, :].astype(jnp.float32) * s[h : h + 1, :] for ref, s in zip(refs, shares)],
            )
        )
    return jnp.concatenate(heads, axis=0), top + jnp.log2(total)


def merge_into(out, refs):
    both, lse = merged(refs)
    out[0:128, :] = both.astype(jnp.bfloat16)
    out[128:PACK, :] = split_lse(lse)


def reduce_and_mix(wire, peers, a, got, mix, x_ref, weights, gain, bias):
    zp, zm, xq = peers
    w_out, w_up, w_down, ready = weights

    def slot(dx, dz, j, n=1):
        return a.at[dx * 4 + dz, pl.ds(j, n)] if n > 1 else a.at[dx * 4 + dz, j]

    def run(ref, j, n=1):
        return ref.at[pl.ds(j, n)] if n > 1 else ref.at[j]

    for j in (0, 2, 1, 3):
        wire.send(("x2", j), slot(1, 2, j), run(got, j), xq)
    for h in range(2):
        wire.send(("pm", h), slot(1, 1, 2 * h, 2), run(got, 4 + 2 * h, 2), zp)
        wire.send(("mm", h), slot(1, 3, 2 * h, 2), run(got, 8 + 2 * h, 2), zm)
    for j in (0, 2, 1, 3):
        wire.arrived(("x2", j))
        merge_into(run(mix, j), [run(got, j), slot(0, 2, j)])
        wire.send(("c", j), run(mix, j), run(got, 12 + j), zp if j in PLUS else zm)
    wire.send("zp", slot(0, 1, 2, 2), run(got, 18, 2), zp)
    wire.send("zm", slot(0, 3, 0, 2), run(got, 20, 2), zm)
    for h in range(2):
        wire.arrived(("pm", h))
        wire.arrived(("mm", h))
        for j in (2 * h, 2 * h + 1):
            merge_into(run(mix, 4 + j), [run(got, 4 + j), run(got, 8 + j), slot(1, 0, j)])
        wire.send(("x", h), run(mix, 4 + 2 * h, 2), run(got, 24 + 2 * h, 2), xq)
    for j in (0, 2, 1, 3):
        wire.arrived(("c", j))
        if j in PLUS:
            merge_into(run(mix, 8 + j), [run(got, 12 + j), slot(0, 1, j)])
            wire.send(("z", j), run(mix, 8 + j), run(got, 16 + j), zp)
        else:
            merge_into(run(mix, 8 + j), [run(got, 12 + j), slot(0, 3, j)])
            wire.send(("z", j), run(mix, 8 + j), run(got, 20 + j), zm)
    for i in ready:
        i.wait()
    mixed = x_ref[...].astype(jnp.float32)
    wire.arrived("zp")
    wire.arrived("zm")
    wire.arrived(("x", 0))
    wire.arrived(("x", 1))
    for j in (0, 2, 1, 3):
        wire.arrived(("z", j))
        both, _ = merged([run(got, 16 + j), run(got, 20 + j), run(got, 24 + j), slot(0, 0, j)])
        attn = jnp.transpose(both).astype(jnp.bfloat16)
        mixed = mixed + dot_nn(attn, w_out[128 * j : 128 * j + 128, :])
    hidden = layer_norm(mixed, gain[0:1], bias[0:1]).astype(jnp.bfloat16)
    up = jax.nn.gelu(dot_nn(hidden, w_up[...])).astype(jnp.bfloat16)
    down = dot_nn(up, w_down[...])
    return layer_norm(hidden.astype(jnp.float32) + down, gain[1:2], bias[1:2]).astype(jnp.bfloat16)


def gather_and_project(
    wire, peers, x_ref, xg, qg, w, wvt, ready, aside, q_ref, k_ref, vt_ref
):
    zp, zm, xq, yp, ym, xk, sib = peers

    def part(ref, j, n=1):
        return ref.at[pl.ds(32 * j, 32 * n)]

    def key(c, dx, dy, j=0, n=4):
        return xg.at[c * 8 + dx * 4 + dy, pl.ds(32 * j, 32 * n)]

    def query(dx, dz, j=0, n=4):
        return qg.at[dx * 4 + dz, pl.ds(128 * j, 128 * n)]

    def across(dx, dy, j=0, n=4):
        wire.send(("s", dx, dy, j), key(0, dx, dy, j, n), key(1, dx, dy, j, n), sib)

    for i in range(4):
        j = (i + 2) % 4
        wire.send(("k", 0, 3, i), part(x_ref, i), key(0, 0, 3, i, 1), yp)
        wire.send(("k", 0, 1, j), part(x_ref, j), key(0, 0, 1, j, 1), ym)
        if i % 2 == 0:
            wire.send(("k", 1, 0, i), part(x_ref, i, 2), key(0, 1, 0, i, 2), xk)
    wire.send(("s", 0, 0, 0), part(x_ref, 0, 4), key(1, 0, 0), sib)
    for i in ready:
        i.wait()
    q = dot_nn(x_ref[...], w[:, 0:512]) * (0.125 * LOG2E)
    for i in range(4):
        qg[0, 128 * i : 128 * i + 128, :] = jnp.transpose(q[:, 128 * i : 128 * i + 128]).astype(
            jnp.bfloat16
        )
    for i in range(4):
        j = (i + 2) % 4
        wire.send(("q", 0, 3, i), query(0, 0, i, 1), query(0, 3, i, 1), zp)
        wire.send(("q", 0, 1, j), query(0, 0, j, 1), query(0, 1, j, 1), zm)
        if i % 2 == 0:
            wire.send(("q", 1, 0, i), query(0, 0, i, 2), query(1, 0, i, 2), xq)
    wvt[...] = jnp.transpose(w[:, 1024:1536].astype(jnp.float32)).astype(jnp.bfloat16)
    off = jnp.zeros((64, 128), jnp.bfloat16)
    for s in range(NQ):
        for p in range(4):
            q_ref[s, p, 0:64, 128:256] = off
            q_ref[s, p, 64:128, 0:128] = off
    if aside is not None:
        aside()

    def project(slots):
        rows = jnp.concatenate([x_ref[...] if s == 0 else xg[s] for s in slots], axis=0)
        keys = dot_nn(rows, w[:, 512:1024]).astype(jnp.bfloat16)
        values = dot_nt(wvt[...], rows).astype(jnp.bfloat16)
        for i, s in enumerate(slots):
            k_ref[s] = keys[128 * i : 128 * i + 128]
            vt_ref[s] = values[:, 128 * i : 128 * i + 128]

    def spread_query(s):
        for p in range(4):
            q_ref[s, p, 0:64, 0:128] = qg[s, 128 * p : 128 * p + 64, :]
            q_ref[s, p, 64:128, 128:256] = qg[s, 128 * p + 64 : 128 * p + 128, :]

    for i in range(2):
        wire.arrived(("k", 0, 3, i))
        wire.send(("k", 0, 2, i), key(0, 0, 3, i, 1), key(0, 0, 2, i, 1), yp)
        wire.arrived(("k", 0, 1, 2 + i))
        wire.send(("k", 0, 2, 2 + i), key(0, 0, 1, 2 + i, 1), key(0, 0, 2, 2 + i, 1), ym)
    for i in (0, 2):
        wire.arrived(("k", 1, 0, i))
        wire.send(("k", 1, 3, i), key(0, 1, 0, i, 2), key(0, 1, 3, i, 2), yp)
        wire.send(("k", 1, 1, i), key(0, 1, 0, i, 2), key(0, 1, 1, i, 2), ym)
    for i in range(2):
        wire.arrived(("q", 0, 3, i))
        wire.send(("q", 0, 2, i), query(0, 3, i, 1), query(0, 2, i, 1), zp)
        wire.arrived(("q", 0, 1, 2 + i))
        wire.send(("q", 0, 2, 2 + i), query(0, 1, 2 + i, 1), query(0, 2, 2 + i, 1), zm)
    for i in (0, 2):
        wire.arrived(("q", 1, 0, i))
        wire.send(("q", 1, 3, i), query(1, 0, i, 2), query(1, 3, i, 2), zp)
        wire.send(("q", 1, 1, i), query(1, 0, i, 2), query(1, 1, i, 2), zm)
    across(1, 0)
    for i in range(2):
        wire.arrived(("k", 0, 3, 2 + i))
        wire.arrived(("k", 0, 1, i))
    across(0, 3)
    across(0, 1)
    wire.arrived(("s", 0, 0, 0))
    project((0, 8))
    for j in (0, 2, 1, 3):
        wire.arrived(("k", 0, 2, j))
        wire.send(("k", 1, 2, j), key(0, 0, 2, j, 1), key(0, 1, 2, j, 1), xk)
    across(0, 2)
    for j in (0, 2, 1, 3):
        wire.arrived(("q", 0, 2, j))
        wire.send(("q", 1, 2, j), query(0, 2, j, 1), query(1, 2, j, 1), xq)
    project((1, 3))
    project((2, 4))
    for i in range(2):
        wire.arrived(("q", 0, 3, 2 + i))
        wire.arrived(("q", 0, 1, i))
    for dz in range(4):
        spread_query(dz)
    for dx, dy in ((1, 0), (0, 3), (0, 1), (0, 2)):
        wire.arrived(("s", dx, dy, 0))
    project((9, 11))
    for i in (0, 2):
        for dy in (1, 3):
            wire.arrived(("k", 1, dy, i))
            across(1, dy, i, 2)
    project((10, 12))
    for j in (0, 2, 1, 3):
        wire.arrived(("k", 1, 2, j))
        across(1, 2, j, 1)
    project((5, 7))
    for i in (0, 2):
        for dy in (1, 3):
            wire.arrived(("s", 1, dy, i))
    project((13, 15))
    for j in (0, 2, 1, 3):
        wire.arrived(("s", 1, 2, j))
    project((6, 14))
    for i in (0, 2):
        for dz in (1, 3):
            wire.arrived(("q", 1, dz, i))
    for j in range(4):
        wire.arrived(("q", 1, 2, j))
    for dz in range(4):
        spread_query(4 + dz)


def link_kernel(layer, reduces, gathers, *refs):
    refs = list(refs)
    x_ref = refs.pop(0)
    starts = not reduces
    if reduces:
        sums = refs[:3]
        w_out_h, w_up_h, w_down_h, gain_ref, bias_ref = refs[3:8]
        refs = refs[8:]
    if gathers:
        w_h = refs.pop(0)
    if starts:
        mask_h = refs.pop(0)
    if reduces:
        x_out = refs.pop(0)
    if gathers:
        q_ref, k_ref, vt_ref = refs[:3]
        refs = refs[3:]
    if starts:
        sub_ref = refs.pop(0)
        mask, x_own = refs[-2:]
        refs = refs[:-2]
    send_sem, recv_sem, copy_sem = refs[:3]
    refs = refs[3:]
    place = Place()
    peers = [
        place.at(z=place.z + 1),
        place.at(z=place.z + 3),
        place.at(x=3 - place.x),
    ]
    if gathers:
        peers += [
            place.at(y=place.y + 1),
            place.at(y=place.y + 3),
            place.at(x=place.x + 1 - 2 * (place.x % 2)),
            place.at(core=1 - place.core),
        ]
    copies = []

    def load(src, dst):
        copy = pltpu.make_async_copy(src, dst, copy_sem.at[len(copies)])
        copy.start()
        copies.append(copy)
        return copy

    if starts:
        x_ready = load(x_ref, x_own)
        x_ref = x_own
    if reduces:
        a_ref, got, mix, w_out, w_up, w_down = refs[:6]
        refs = refs[6:]
        mix_ready = [
            load(w_out_h.at[layer], w_out),
            load(w_up_h.at[layer], w_up),
            load(w_down_h.at[layer], w_down),
        ]
    if gathers:
        xg, qg, w, wvt = refs
        w_ready = [load(w_h.at[layer + 1], w)]
    if starts:
        mask_ready = load(mask_h, mask)
    barrier = pltpu.get_barrier_semaphore()
    for peer in peers:
        pl.semaphore_signal(barrier, inc=1, device_id=peer, device_id_type=MESH)
    if reduces:
        finish_parts(*sums, a_ref)
    pl.semaphore_wait(barrier, len(peers))
    wire = Wire(send_sem, recv_sem)
    if starts:
        x_ready.wait()
    if reduces:
        x_out[...] = reduce_and_mix(
            wire, peers[:3], a_ref, got, mix, x_ref, (w_out, w_up, w_down, mix_ready),
            gain_ref[layer], bias_ref[layer],
        )
        x_ref = x_out
    def slice_mask():
        mask_ready.wait()
        queries, keys = query_blocks(place), key_blocks(place)
        for i in range(NQ):
            for j in range(NK):
                sub_ref[i, j] = mask[queries[i], keys[j]]

    if gathers:
        gather_and_project(
            wire, peers, x_ref, xg, qg, w, wvt, w_ready, slice_mask if starts else None, q_ref, k_ref, vt_ref
        )
    wire.drain()


def link(layer, x, reduce_args=None, w_qkv=None, block_mask=None):
    reduces, gathers = reduce_args is not None, w_qkv is not None
    vmem = pl.BlockSpec(memory_space=pltpu.VMEM)
    hbm = pl.BlockSpec(memory_space=pltpu.HBM)
    args, specs, outs = [x], [vmem if reduces else hbm], []
    scratch = [
        pltpu.SemaphoreType.DMA((20 * reduces + 57 * gathers,)),
        pltpu.SemaphoreType.DMA((20 * reduces + 57 * gathers,)),
        pltpu.SemaphoreType.DMA((4,)),
    ]
    bf16 = jnp.bfloat16
    if reduces:
        args += list(reduce_args)
        specs += [vmem, vmem, vmem, hbm, hbm, hbm, vmem, vmem]
        outs.append(jax.ShapeDtypeStruct((128, 512), bf16))
        scratch += [
            pltpu.VMEM((NQ, 4, PACK, 128), bf16),
            pltpu.VMEM((28, PACK, 128), bf16),
            pltpu.VMEM((12, PACK, 128), bf16),
            pltpu.VMEM((512, 512), bf16),
            pltpu.VMEM((512, 1024), bf16),
            pltpu.VMEM((1024, 512), bf16),
        ]
    if gathers:
        args.append(w_qkv)
        specs.append(hbm)
        outs += [
            pltpu.VMEM((NQ, 4, 128, 256), bf16),
            pltpu.VMEM((NK, 128, 512), bf16),
            pltpu.VMEM((NK, 512, 128), bf16),
        ]
        scratch += [
            pltpu.VMEM((NK, 128, 512), bf16),
            pltpu.VMEM((NQ, 512, 128), bf16),
            pltpu.VMEM((512, 1536), bf16),
            pltpu.VMEM((512, 512), bf16),
        ]
    out_specs = [vmem for _ in outs]
    if not reduces:
        args.append(block_mask)
        specs.append(hbm)
        outs.append(jax.ShapeDtypeStruct((NQ, NK), jnp.int32))
        out_specs.append(pl.BlockSpec(memory_space=pltpu.SMEM))
        scratch += [pltpu.SMEM((128, 128), jnp.int32), pltpu.VMEM((128, 512), bf16)]
    return pl.pallas_call(
        functools.partial(link_kernel, layer, reduces, gathers),
        out_shape=tuple(outs),
        in_specs=specs,
        out_specs=tuple(out_specs),
        scratch_shapes=scratch,
        compiler_params=pltpu.CompilerParams(
            collective_id=layer + 1, has_side_effects=True, vmem_limit_bytes=24 * 2**20
        ),
    )(*args)


def per_device(node_feats, block_mask, w_qkv, w_out, w_up, w_down, ln_gain, ln_bias):
    x = node_feats
    w_qkv, w_out, w_up, w_down, block_mask = (
        pltpu.with_memory_space_constraint(a, pltpu.HBM)
        for a in (w_qkv, w_out, w_up, w_down, block_mask)
    )
    x_first = pltpu.with_memory_space_constraint(x, pltpu.HBM)
    q, k, vt, sub = link(-1, x_first, w_qkv=w_qkv, block_mask=block_mask)
    for layer in range(LAYERS):
        parts = attention(sub, q, k, vt)
        last = layer == LAYERS - 1
        rest = (*parts, w_out, w_up, w_down, ln_gain, ln_bias)
        if last:
            (x,) = link(layer, x, reduce_args=rest)
        else:
            x, q, k, vt = link(layer, x, reduce_args=rest, w_qkv=w_qkv)
    return x


def solution(mesh):
    placed = (P(("row", "col"), None), P(), P(), P(), P(), P(), P(), P())
    return jax.shard_map(
        per_device, mesh=mesh, in_specs=placed, out_specs=P(("row", "col"), None), check_vma=False
    )
```

```python
import functools

import jax
import jax.numpy as jnp
from jax import lax
from jax.experimental import pallas as pl
from jax.experimental.pallas import tpu as pltpu
from jax.sharding import PartitionSpec as P

HEADS = 8
BLOCK = 128
LAYERS = 2
NQ = 8
NK = 16
LOG2E = 1.4426950408889634
LOW = -1e30
PACK = 144
PLUS, MINUS = (0, 1), (2, 3)
MESH = pl.DeviceIdType.MESH


def dot_nn(a, b):
    return lax.dot_general(a, b, (((1,), (0,)), ((), ())), preferred_element_type=jnp.float32)


def dot_nt(a, b):
    return lax.dot_general(a, b, (((1,), (1,)), ((), ())), preferred_element_type=jnp.float32)


def layer_norm(values, gain, bias):
    center = values - jnp.mean(values, axis=-1, keepdims=True)
    spread = jnp.mean(center * center, axis=-1, keepdims=True)
    return center * lax.rsqrt(spread + 1e-05) * gain + bias


def split_lse(lse):
    high = lse.astype(jnp.bfloat16).astype(jnp.float32)
    rest = lse - high
    mid = rest.astype(jnp.bfloat16).astype(jnp.float32)
    low = rest - mid
    pad = jnp.zeros((10, 128), jnp.float32)
    return jnp.concatenate([high, mid, low, pad], axis=0).astype(jnp.bfloat16)


def joined_lse(ref):
    parts = ref[128:PACK, :].astype(jnp.float32)
    return parts[0:2] + parts[2:4] + parts[4:6]


def finish_parts(peaks, masses, acc, a_ref):
    for r in range(NQ):
        mass, peak = masses[r], peaks[r]
        some = mass > 0.0
        safe = jnp.where(some, mass, 1.0)
        inv = jnp.where(some, 1.0 / safe, 0.0)
        lse = jnp.where(some, peak + jnp.log2(safe), LOW)
        for p in range(4):
            for h in range(2):
                rows = slice(128 * p + 64 * h, 128 * p + 64 * h + 64)
                side = slice(128 * h, 128 * h + 128)
                a_ref[r, p, 64 * h : 64 * h + 64, :] = (
                    acc[r, rows, :] * inv[p : p + 1, side]
                ).astype(jnp.bfloat16)
            pair = jnp.concatenate([lse[p : p + 1, :128], lse[p : p + 1, 128:]], axis=0)
            a_ref[r, p, 128:PACK, :] = split_lse(pair)


def attention_kernel(
    sub_any, qd, k_ref, vt_ref, peaks, masses, acc,
    sub_ref, sub_sem, order, scores_a, scores_b, tops_a, tops_b,
):
    sub_copy = pltpu.make_async_copy(sub_any, sub_ref, sub_sem)
    sub_copy.start()
    peaks[...] = jnp.full_like(peaks, LOW)
    masses[...] = jnp.zeros_like(masses)
    acc[...] = jnp.zeros_like(acc)
    sub_copy.wait()
    bank = ((scores_a, tops_a), (scores_b, tops_b))
    count = jnp.int32(0)
    for r in range(NQ):
        for k in range(NK):
            order[count] = 32 * r + k
            count = count + sub_ref[r, k]
        order[count] = order[jnp.maximum(count - 1, 0)] + 16
        count = count + count % 2
    units = count // 2
    last = jnp.maximum(count - 1, 0)
    tail = order[last]
    order[count] = tail - tail % 32 + tail % 16 + 16
    order[count + 1] = order[count]

    def decode(u):
        first, second = order[2 * u], order[2 * u + 1]
        dead = [jnp.where((code // 16) % 2 == 1, LOW, 0.0) for code in (first, second)]
        return first // 32, first % 16, second % 16, dead

    def score(u, slot, p):
        r, k0, k1, dead = decode(u)
        scores, tops = bank[slot]
        lanes = slice(128 * p, 128 * p + 128)
        keys = jnp.concatenate([k_ref[k0, :, lanes], k_ref[k1, :, lanes]], axis=0)
        s = dot_nn(keys, qd[r, p])
        scores[p] = s
        top = jnp.maximum(
            jnp.max(s[0:128], axis=0, keepdims=True) + dead[0],
            jnp.max(s[128:256], axis=0, keepdims=True) + dead[1],
        )
        tops[p : p + 1, :] = top

    def absorb(u, slot, p):
        r, k0, k1, dead = decode(u)
        scores, tops = bank[slot]
        before = peaks[r, p : p + 1, :]
        here = jnp.maximum(before, tops[p : p + 1, :])
        fade = jnp.exp2(before - here)
        peaks[r, p : p + 1, :] = here
        lanes = slice(128 * p, 128 * p + 128)
        w0 = jnp.exp2(scores[p, 0:128] - (here - dead[0]))
        w1 = jnp.exp2(scores[p, 128:256] - (here - dead[1]))
        mass = jnp.sum(w0, axis=0, keepdims=True) + jnp.sum(w1, axis=0, keepdims=True)
        w = jnp.concatenate([w0.astype(jnp.bfloat16), w1.astype(jnp.bfloat16)], axis=0)
        values = jnp.concatenate([vt_ref[k0, lanes, :], vt_ref[k1, lanes, :]], axis=1)
        o = dot_nn(values, w)
        lo, hi = slice(128 * p, 128 * p + 64), slice(128 * p + 64, 128 * p + 128)
        acc[r, lo, :] = acc[r, lo, :] * fade[:, :128] + o[0:64, 0:128]
        acc[r, hi, :] = acc[r, hi, :] * fade[:, 128:] + o[64:128, 128:256]
        masses[r, p : p + 1, :] = masses[r, p : p + 1, :] * fade + mass

    for p in range(4):
        score(0, 0, p)

    def two_units(i, carry):
        u = 2 * i
        for p in range(4):
            score(u + 1, 1, p)
            absorb(u, 0, p)
        for p in range(4):
            score(jnp.minimum(u + 2, units), 0, p)
            absorb(u + 1, 1, p)
        return carry

    lax.fori_loop(0, (units + 1) // 2, two_units, 0)


def attention(sub, q, k, vt):
    vmem = pl.BlockSpec(memory_space=pltpu.VMEM)
    return pl.pallas_call(
        attention_kernel,
        out_shape=(
            pltpu.VMEM((NQ, 4, 256), jnp.float32),
            pltpu.VMEM((NQ, 4, 256), jnp.float32),
            pltpu.VMEM((NQ, 512, 128), jnp.float32),
        ),
        in_specs=[pl.BlockSpec(memory_space=pl.ANY), vmem, vmem, vmem],
        out_specs=(vmem, vmem, vmem),
        scratch_shapes=[
            pltpu.SMEM((NQ, NK), jnp.int32),
            pltpu.SemaphoreType.DMA,
            pltpu.SMEM((NQ * NK + 4,), jnp.int32),
            pltpu.VMEM((4, 256, 256), jnp.float32),
            pltpu.VMEM((4, 256, 256), jnp.float32),
            pltpu.VMEM((4, 256), jnp.float32),
            pltpu.VMEM((4, 256), jnp.float32),
        ],
        compiler_params=pltpu.CompilerParams(vmem_limit_bytes=16 * 2**20),
    )(sub, q, k, vt)


class Place:
    def __init__(self):
        row, col = lax.axis_index("row"), lax.axis_index("col")
        self.z, self.y, self.core = row // 2, col // 4, col % 2
        self.x = (row % 2) * 2 + (col // 2) % 2

    def at(self, x=None, y=None, z=None, core=None):
        x = self.x if x is None else x
        y = self.y if y is None else y % 4
        z = self.z if z is None else z % 4
        core = self.core if core is None else core
        return (z * 2 + x // 2, (y * 2 + x % 2) * 2 + core)


def key_blocks(place):
    out = []
    for c in range(2):
        for dx in range(2):
            for dy in range(4):
                x = place.x if dx == 0 else place.x + 1 - 2 * (place.x % 2)
                core = place.core if c == 0 else 1 - place.core
                row, col = place.at(x=x, y=place.y + dy, core=core)
                out.append(row * 16 + col)
    return out


def query_blocks(place):
    out = []
    for dx in range(2):
        for dz in range(4):
            x = place.x if dx == 0 else 3 - place.x
            row, col = place.at(x=x, z=place.z + dz)
            out.append(row * 16 + col)
    return out


class Wire:
    def __init__(self, send_sem, recv_sem):
        self.send_sem, self.recv_sem, self.copies = send_sem, recv_sem, {}

    def send(self, name, src, dst, to):
        m = len(self.copies)
        copy = pltpu.make_async_remote_copy(
            src_ref=src,
            dst_ref=dst,
            send_sem=self.send_sem.at[m],
            recv_sem=self.recv_sem.at[m],
            device_id=to,
            device_id_type=MESH,
        )
        copy.start()
        self.copies[name] = copy

    def arrived(self, name):
        self.copies[name].wait_recv()

    def drain(self):
        for copy in self.copies.values():
            copy.wait_send()


def merged(refs):
    lses = [joined_lse(ref) for ref in refs]
    top = functools.reduce(jnp.maximum, lses)
    parts = [jnp.exp2(lse - top) for lse in lses]
    total = functools.reduce(jnp.add, parts)
    shares = [part / total for part in parts]
    heads = []
    for h in range(2):
        rows = slice(64 * h, 64 * h + 64)
        heads.append(
            functools.reduce(
                jnp.add,
                [ref[rows, :].astype(jnp.float32) * s[h : h + 1, :] for ref, s in zip(refs, shares)],
            )
        )
    return jnp.concatenate(heads, axis=0), top + jnp.log2(total)


def merge_into(out, refs):
    both, lse = merged(refs)
    out[0:128, :] = both.astype(jnp.bfloat16)
    out[128:PACK, :] = split_lse(lse)


def reduce_and_mix(wire, peers, a, got, mix, x_ref, weights, gain, bias):
    zp, zm, xq = peers
    w_out, w_up, w_down, ready = weights

    def slot(dx, dz, j, n=1):
        return a.at[dx * 4 + dz, pl.ds(j, n)] if n > 1 else a.at[dx * 4 + dz, j]

    def run(ref, j, n=1):
        return ref.at[pl.ds(j, n)] if n > 1 else ref.at[j]

    for j in (0, 2, 1, 3):
        wire.send(("x2", j), slot(1, 2, j), run(got, j), xq)
    for h in range(2):
        wire.send(("pm", h), slot(1, 1, 2 * h, 2), run(got, 4 + 2 * h, 2), zp)
        wire.send(("mm", h), slot(1, 3, 2 * h, 2), run(got, 8 + 2 * h, 2), zm)
    for j in (0, 2, 1, 3):
        wire.arrived(("x2", j))
        merge_into(run(mix, j), [run(got, j), slot(0, 2, j)])
        wire.send(("c", j), run(mix, j), run(got, 12 + j), zp if j in PLUS else zm)
    wire.send("zp", slot(0, 1, 2, 2), run(got, 18, 2), zp)
    wire.send("zm", slot(0, 3, 0, 2), run(got, 20, 2), zm)
    for h in range(2):
        wire.arrived(("pm", h))
        wire.arrived(("mm", h))
        for j in (2 * h, 2 * h + 1):
            merge_into(run(mix, 4 + j), [run(got, 4 + j), run(got, 8 + j), slot(1, 0, j)])
        wire.send(("x", h), run(mix, 4 + 2 * h, 2), run(got, 24 + 2 * h, 2), xq)
    for j in (0, 2, 1, 3):
        wire.arrived(("c", j))
        if j in PLUS:
            merge_into(run(mix, 8 + j), [run(got, 12 + j), slot(0, 1, j)])
            wire.send(("z", j), run(mix, 8 + j), run(got, 16 + j), zp)
        else:
            merge_into(run(mix, 8 + j), [run(got, 12 + j), slot(0, 3, j)])
            wire.send(("z", j), run(mix, 8 + j), run(got, 20 + j), zm)
    for i in ready:
        i.wait()
    mixed = x_ref[...].astype(jnp.float32)
    wire.arrived("zp")
    wire.arrived("zm")
    wire.arrived(("x", 0))
    wire.arrived(("x", 1))
    for j in (0, 2, 1, 3):
        wire.arrived(("z", j))
        both, _ = merged([run(got, 16 + j), run(got, 20 + j), run(got, 24 + j), slot(0, 0, j)])
        attn = jnp.transpose(both).astype(jnp.bfloat16)
        mixed = mixed + dot_nn(attn, w_out[128 * j : 128 * j + 128, :])
    hidden = layer_norm(mixed, gain[0:1], bias[0:1]).astype(jnp.bfloat16)
    up = jax.nn.gelu(dot_nn(hidden, w_up[...])).astype(jnp.bfloat16)
    down = dot_nn(up, w_down[...])
    return layer_norm(hidden.astype(jnp.float32) + down, gain[1:2], bias[1:2]).astype(jnp.bfloat16)


def gather_and_project(
    wire, peers, x_ref, xg, qg, w, wvt, ready, aside, q_ref, k_ref, vt_ref
):
    zp, zm, xq, yp, ym, xk, sib, yf, zf = peers

    def part(ref, j, n=1):
        return ref.at[pl.ds(32 * j, 32 * n)]

    def key(c, dx, dy, j=0, n=4):
        return xg.at[c * 8 + dx * 4 + dy, pl.ds(32 * j, 32 * n)]

    def query(dx, dz, j=0, n=4):
        return qg.at[dx * 4 + dz, pl.ds(128 * j, 128 * n)]

    def across(dx, dy, j=0, n=4):
        wire.send(("s", dx, dy, j), key(0, dx, dy, j, n), key(1, dx, dy, j, n), sib)

    def start(name, source, at, far, plus, minus, pair):
        for d, h, to in ((2, 0, far), (0, 2, pair), (3, 0, plus), (1, 0, minus),
                         (0, 0, pair), (2, 2, far), (3, 2, plus), (1, 2, minus)):
            dx = 1 if d == 0 else 0
            wire.send((name, dx, d, h), source(h), at(dx, d, h, 2), to)

    def relay(name, at, far, plus, minus, pair):
        wire.arrived((name, 1, 0, 2))
        for d, to in ((2, far), (3, plus), (1, minus)):
            wire.send((name, 1, d, 2), at(1, 0, 2, 2), at(1, d, 2, 2), to)

    def relay_pair(name, at, pair):
        for d in (2, 3, 1):
            wire.arrived((name, 0, d, 0))
            wire.send((name, 1, d, 0), at(0, d, 0, 2), at(1, d, 0, 2), pair)

    def key0(dx, dy, j, n):
        return key(0, dx, dy, j, n)

    start("k", lambda h: part(x_ref, h, 2), key0, yf, yp, ym, xk)
    wire.send(("s", 0, 0, 0), part(x_ref, 0, 4), key(1, 0, 0), sib)
    for i in ready:
        i.wait()
    q = dot_nn(x_ref[...], w[:, 0:512]) * (0.125 * LOG2E)
    for i in range(4):
        qg[0, 128 * i : 128 * i + 128, :] = jnp.transpose(q[:, 128 * i : 128 * i + 128]).astype(
            jnp.bfloat16
        )
    start("q", lambda h: query(0, 0, h, 2), query, zf, zp, zm, xq)
    wvt[...] = jnp.transpose(w[:, 1024:1536].astype(jnp.float32)).astype(jnp.bfloat16)
    off = jnp.zeros((64, 128), jnp.bfloat16)
    for s in range(NQ):
        for p in range(4):
            q_ref[s, p, 0:64, 128:256] = off
            q_ref[s, p, 64:128, 0:128] = off
    if aside is not None:
        aside()

    def project(slots):
        rows = jnp.concatenate([x_ref[...] if s == 0 else xg[s] for s in slots], axis=0)
        keys = dot_nn(rows, w[:, 512:1024]).astype(jnp.bfloat16)
        values = dot_nt(wvt[...], rows).astype(jnp.bfloat16)
        for i, s in enumerate(slots):
            k_ref[s] = keys[128 * i : 128 * i + 128]
            vt_ref[s] = values[:, 128 * i : 128 * i + 128]

    def spread_query(s):
        for p in range(4):
            q_ref[s, p, 0:64, 0:128] = qg[s, 128 * p : 128 * p + 64, :]
            q_ref[s, p, 64:128, 128:256] = qg[s, 128 * p + 64 : 128 * p + 128, :]

    relay("k", key0, yf, yp, ym, xk)
    relay("q", query, zf, zp, zm, xq)
    relay_pair("k", key0, xk)
    relay_pair("q", query, xq)
    wire.arrived(("k", 1, 0, 0))
    across(1, 0)
    for d in (2, 3, 1):
        wire.arrived(("k", 0, d, 2))
        across(0, d)
    wire.arrived(("s", 0, 0, 0))
    project((0, 8))
    project((1, 3))
    project((2, 4))
    for h in (2, 0):
        for d in (2, 3, 1):
            wire.arrived(("k", 1, d, h))
            across(1, d, h, 2)
    wire.arrived(("q", 1, 0, 0))
    for d in (2, 3, 1):
        wire.arrived(("q", 0, d, 2))
    for dz in range(4):
        spread_query(dz)
    for dx, dy in ((1, 0), (0, 3), (0, 1), (0, 2)):
        wire.arrived(("s", dx, dy, 0))
    project((9, 11))
    project((10, 12))
    project((5, 7))
    for h in (2, 0):
        for d in (1, 3):
            wire.arrived(("s", 1, d, h))
    project((13, 15))
    for h in (2, 0):
        wire.arrived(("s", 1, 2, h))
    project((6, 14))
    for h in (2, 0):
        for d in (2, 3, 1):
            wire.arrived(("q", 1, d, h))
    for dz in range(4):
        spread_query(4 + dz)


def link_kernel(layer, reduces, gathers, *refs):
    refs = list(refs)
    x_ref = refs.pop(0)
    starts = not reduces
    if reduces:
        sums = refs[:3]
        w_out_h, w_up_h, w_down_h, gain_ref, bias_ref = refs[3:8]
        refs = refs[8:]
    if gathers:
        w_h = refs.pop(0)
    if starts:
        mask_h = refs.pop(0)
    if reduces:
        x_out = refs.pop(0)
    if gathers:
        q_ref, k_ref, vt_ref = refs[:3]
        refs = refs[3:]
    if starts:
        sub_ref = refs.pop(0)
        mask, x_own = refs[-2:]
        refs = refs[:-2]
    send_sem, recv_sem, copy_sem = refs[:3]
    refs = refs[3:]
    place = Place()
    peers = [
        place.at(z=place.z + 1),
        place.at(z=place.z + 3),
        place.at(x=3 - place.x),
    ]
    if gathers:
        peers += [
            place.at(y=place.y + 1),
            place.at(y=place.y + 3),
            place.at(x=place.x + 1 - 2 * (place.x % 2)),
            place.at(core=1 - place.core),
            place.at(y=place.y + 2),
            place.at(z=place.z + 2),
        ]
    copies = []

    def load(src, dst):
        copy = pltpu.make_async_copy(src, dst, copy_sem.at[len(copies)])
        copy.start()
        copies.append(copy)
        return copy

    if starts:
        x_ready = load(x_ref, x_own)
        x_ref = x_own
    if reduces:
        a_ref, got, mix, w_out, w_up, w_down = refs[:6]
        refs = refs[6:]
        mix_ready = [
            load(w_out_h.at[layer], w_out),
            load(w_up_h.at[layer], w_up),
            load(w_down_h.at[layer], w_down),
        ]
    if gathers:
        xg, qg, w, wvt = refs
        w_ready = [load(w_h.at[layer + 1], w)]
    if starts:
        mask_ready = load(mask_h, mask)
    barrier = pltpu.get_barrier_semaphore()
    for peer in peers:
        pl.semaphore_signal(barrier, inc=1, device_id=peer, device_id_type=MESH)
    if reduces:
        finish_parts(*sums, a_ref)
    pl.semaphore_wait(barrier, len(peers))
    wire = Wire(send_sem, recv_sem)
    if starts:
        x_ready.wait()
    if reduces:
        x_out[...] = reduce_and_mix(
            wire, peers[:3], a_ref, got, mix, x_ref, (w_out, w_up, w_down, mix_ready),
            gain_ref[layer], bias_ref[layer],
        )
        x_ref = x_out
    def slice_mask():
        mask_ready.wait()
        queries, keys = query_blocks(place), key_blocks(place)
        for i in range(NQ):
            for j in range(NK):
                sub_ref[i, j] = mask[queries[i], keys[j]]

    if gathers:
        gather_and_project(
            wire, peers, x_ref, xg, qg, w, wvt, w_ready, slice_mask if starts else None, q_ref, k_ref, vt_ref
        )
    wire.drain()


def link(layer, x, reduce_args=None, w_qkv=None, block_mask=None):
    reduces, gathers = reduce_args is not None, w_qkv is not None
    vmem = pl.BlockSpec(memory_space=pltpu.VMEM)
    hbm = pl.BlockSpec(memory_space=pltpu.HBM)
    args, specs, outs = [x], [vmem if reduces else hbm], []
    scratch = [
        pltpu.SemaphoreType.DMA((20 * reduces + 41 * gathers,)),
        pltpu.SemaphoreType.DMA((20 * reduces + 41 * gathers,)),
        pltpu.SemaphoreType.DMA((4,)),
    ]
    bf16 = jnp.bfloat16
    if reduces:
        args += list(reduce_args)
        specs += [vmem, vmem, vmem, hbm, hbm, hbm, vmem, vmem]
        outs.append(jax.ShapeDtypeStruct((128, 512), bf16))
        scratch += [
            pltpu.VMEM((NQ, 4, PACK, 128), bf16),
            pltpu.VMEM((28, PACK, 128), bf16),
            pltpu.VMEM((12, PACK, 128), bf16),
            pltpu.VMEM((512, 512), bf16),
            pltpu.VMEM((512, 1024), bf16),
            pltpu.VMEM((1024, 512), bf16),
        ]
    if gathers:
        args.append(w_qkv)
        specs.append(hbm)
        outs += [
            pltpu.VMEM((NQ, 4, 128, 256), bf16),
            pltpu.VMEM((NK, 128, 512), bf16),
            pltpu.VMEM((NK, 512, 128), bf16),
        ]
        scratch += [
            pltpu.VMEM((NK, 128, 512), bf16),
            pltpu.VMEM((NQ, 512, 128), bf16),
            pltpu.VMEM((512, 1536), bf16),
            pltpu.VMEM((512, 512), bf16),
        ]
    out_specs = [vmem for _ in outs]
    if not reduces:
        args.append(block_mask)
        specs.append(hbm)
        outs.append(jax.ShapeDtypeStruct((NQ, NK), jnp.int32))
        out_specs.append(pl.BlockSpec(memory_space=pltpu.SMEM))
        scratch += [pltpu.SMEM((128, 128), jnp.int32), pltpu.VMEM((128, 512), bf16)]
    return pl.pallas_call(
        functools.partial(link_kernel, layer, reduces, gathers),
        out_shape=tuple(outs),
        in_specs=specs,
        out_specs=tuple(out_specs),
        scratch_shapes=scratch,
        compiler_params=pltpu.CompilerParams(
            collective_id=layer + 1, has_side_effects=True, vmem_limit_bytes=24 * 2**20
        ),
    )(*args)


def per_device(node_feats, block_mask, w_qkv, w_out, w_up, w_down, ln_gain, ln_bias):
    x = node_feats
    w_qkv, w_out, w_up, w_down, block_mask = (
        pltpu.with_memory_space_constraint(a, pltpu.HBM)
        for a in (w_qkv, w_out, w_up, w_down, block_mask)
    )
    x_first = pltpu.with_memory_space_constraint(x, pltpu.HBM)
    q, k, vt, sub = link(-1, x_first, w_qkv=w_qkv, block_mask=block_mask)
    for layer in range(LAYERS):
        parts = attention(sub, q, k, vt)
        last = layer == LAYERS - 1
        rest = (*parts, w_out, w_up, w_down, ln_gain, ln_bias)
        if last:
            (x,) = link(layer, x, reduce_args=rest)
        else:
            x, q, k, vt = link(layer, x, reduce_args=rest, w_qkv=w_qkv)
    return x


def solution(mesh):
    placed = (P(("row", "col"), None), P(), P(), P(), P(), P(), P(), P())
    return jax.shard_map(
        per_device, mesh=mesh, in_specs=placed, out_specs=P(("row", "col"), None), check_vma=False
    )
```
